16 devices in a mesh: dp: 2 (over y, z), tp: 8 (over x, core).
Axes of the slice: x: 4, y: 2, z: 1, core: 2. Of those that a mesh axis runs over, the one named last changes fastest.
The devices are a block of a 4x4x8 slice.
Arguments:
- resid_in: bfloat16 [256, 5120], P('dp'), parts along dimension 0
- positions: int32 [256], P('dp'), parts along dimension 0
- k_cache: bfloat16 [256, 128, 8, 128], P('dp', None, 'tp'), parts along dimension 0
- v_cache: bfloat16 [256, 128, 8, 128], P('dp', None, 'tp'), parts along dimension 0
- gain_attn: bfloat16 [5120], replicated
- w_query: bfloat16 [5120, 4096], P(None, 'tp')
- w_key: bfloat16 [5120, 1024], P(None, 'tp')
- w_value: bfloat16 [5120, 1024], P(None, 'tp')
- w_out: bfloat16 [4096, 5120], P('tp')
- gain_mlp: bfloat16 [5120], replicated
- w_gate: bfloat16 [5120, 32768], P(None, 'tp')
- w_up: bfloat16 [5120, 32768], P(None, 'tp')
- w_down: bfloat16 [32768, 5120], P('tp')
Outputs:
- output 1: bfloat16 [256, 5120], P('dp'), parts along dimension 0
- output 2: bfloat16 [256, 128, 8, 128], P('dp', None, 'tp'), parts along dimension 0
- output 3: bfloat16 [256, 128, 8, 128], P('dp', None, 'tp'), parts along dimension 0
There are 2 independent parts. The reference program is written for one: setup_inputs(seed, part) draws one part's arguments, and reference() takes and returns one part's arrays. A program takes and returns all parts, laid end to end along the dimension named above; an argument that names none is the same for every part.
All inputs are finite; a program needn't handle non-finite values.
Results may differ from the reference program's by a relative error of at most 0.0105374.
Values sent between devices are 32-bit elements.
A program may use at most 768 MiB of HBM per device.

```python
import math
import jax
import jax.numpy as jnp
from jax import lax

BATCH_PART = 128
CACHE_LEN = 128
MODEL_DIM = 5120
Q_HEADS = 32
KV_HEADS = 8
HEAD_DIM = 128
FFN_DIM = 32768

EPS = 1e-5
ROPE_THETA = 500000.0
ROPE_FACTOR = 8.0
LOW_FACTOR = 1.0
HIGH_FACTOR = 4.0
ORIG_CTX = 8192.0


def setup_inputs(seed: int = 0, part: int = 0) -> dict:
    part_keys = jax.random.split(jax.random.fold_in(jax.random.key(seed), part), 6)
    weight_keys = jax.random.split(jax.random.key(seed + 1), 11)
    log_len = int(math.log2(CACHE_LEN))
    dim_scale = 1.0 / math.sqrt(MODEL_DIM)
    out_scale = 1.0 / math.sqrt(Q_HEADS * HEAD_DIM)
    ffn_scale = 1.0 / math.sqrt(FFN_DIM)
    q_width = Q_HEADS * HEAD_DIM
    kv_width = KV_HEADS * HEAD_DIM
    resid_in = jax.random.normal(part_keys[0], (BATCH_PART, MODEL_DIM), jnp.float32)
    exponent = jax.random.randint(part_keys[1], (BATCH_PART,), 0, log_len + 1, dtype=jnp.int32)
    upper_bound = jnp.left_shift(jnp.ones((BATCH_PART,), jnp.int32), exponent)
    positions = jax.random.randint(part_keys[2], (BATCH_PART,), 0, upper_bound, dtype=jnp.int32)
    positions = positions.at[0].set(CACHE_LEN - 1).at[1].set(0)
    cache_shape = (BATCH_PART, CACHE_LEN, KV_HEADS, HEAD_DIM)
    k_cache = jax.random.normal(part_keys[3], cache_shape, jnp.float32)
    v_mean = 0.7 * jax.random.normal(part_keys[4], (BATCH_PART, 1, KV_HEADS, HEAD_DIM), jnp.float32)
    v_cache = v_mean + jax.random.normal(part_keys[5], cache_shape, jnp.float32)
    gain_attn = 1.0 + 0.3 * jax.random.normal(weight_keys[0], (MODEL_DIM,), jnp.float32)
    w_query = jax.random.normal(weight_keys[1], (MODEL_DIM, q_width), jnp.float32) * dim_scale
    w_key = jax.random.normal(weight_keys[2], (MODEL_DIM, kv_width), jnp.float32) * dim_scale
    w_value = jax.random.normal(weight_keys[3], (MODEL_DIM, kv_width), jnp.float32) * dim_scale
    w_out = jax.random.normal(weight_keys[4], (q_width, MODEL_DIM), jnp.float32) * out_scale
    gain_mlp = 1.0 + 0.3 * jax.random.normal(weight_keys[5], (MODEL_DIM,), jnp.float32)
    w_gate = jax.random.normal(weight_keys[6], (MODEL_DIM, FFN_DIM), jnp.float32) * dim_scale
    w_up = jax.random.normal(weight_keys[7], (MODEL_DIM, FFN_DIM), jnp.float32) * dim_scale
    w_down = jax.random.normal(weight_keys[8], (FFN_DIM, MODEL_DIM), jnp.float32) * ffn_scale
    return dict(resid_in=resid_in.astype(jnp.bfloat16), positions=positions,
                k_cache=k_cache.astype(jnp.bfloat16), v_cache=v_cache.astype(jnp.bfloat16),
                gain_attn=gain_attn.astype(jnp.bfloat16), w_query=w_query.astype(jnp.bfloat16),
                w_key=w_key.astype(jnp.bfloat16), w_value=w_value.astype(jnp.bfloat16),
                w_out=w_out.astype(jnp.bfloat16), gain_mlp=gain_mlp.astype(jnp.bfloat16),
                w_gate=w_gate.astype(jnp.bfloat16), w_up=w_up.astype(jnp.bfloat16),
                w_down=w_down.astype(jnp.bfloat16))


def rms_norm(rows_in, gain):
    rows_f = rows_in.astype(jnp.float32)
    mean_sq = jnp.mean(rows_f * rows_f, axis=-1, keepdims=True)
    return (rows_f * lax.rsqrt(mean_sq + EPS) * gain.astype(jnp.float32)).astype(jnp.bfloat16)


def rope_tables(positions, head_dim):
    half_dim = head_dim // 2
    exponents = jnp.arange(half_dim, dtype=jnp.float32) * (2.0 / head_dim)
    inv_freq = 1.0 / jnp.power(ROPE_THETA, exponents)
    wavelen = (2.0 * math.pi) / inv_freq
    smooth = (ORIG_CTX / wavelen - LOW_FACTOR) / (HIGH_FACTOR - LOW_FACTOR)
    blended = (1.0 - smooth) * inv_freq / ROPE_FACTOR + smooth * inv_freq
    inv_freq = jnp.where(wavelen < ORIG_CTX / HIGH_FACTOR, inv_freq,
                         jnp.where(wavelen > ORIG_CTX / LOW_FACTOR, inv_freq / ROPE_FACTOR, blended))
    angles = positions.astype(jnp.float32)[:, None] * inv_freq[None, :]
    return jnp.cos(angles), jnp.sin(angles)


def apply_rope(vectors, cos_t, sin_t):
    half_dim = vectors.shape[-1] // 2
    lower_half = vectors[..., :half_dim]
    upper_half = vectors[..., half_dim:]
    cos_b = cos_t[:, None, :]
    sin_b = sin_t[:, None, :]
    return jnp.concatenate([lower_half * cos_b - upper_half * sin_b,
                            upper_half * cos_b + lower_half * sin_b], axis=-1)


def reference(resid_in, positions, k_cache, v_cache, gain_attn, w_query, w_key, w_value,
              w_out, gain_mlp, w_gate, w_up, w_down):
    group_size = Q_HEADS // KV_HEADS
    n_seqs = resid_in.shape[0]
    normed = rms_norm(resid_in, gain_attn)
    queries = jnp.dot(normed, w_query, preferred_element_type=jnp.float32).astype(jnp.bfloat16)
    key_new = jnp.dot(normed, w_key, preferred_element_type=jnp.float32).astype(jnp.bfloat16)
    value_new = jnp.dot(normed, w_value, preferred_element_type=jnp.float32).astype(jnp.bfloat16)
    cos_t, sin_t = rope_tables(positions, HEAD_DIM)
    queries = apply_rope(queries.reshape(n_seqs, Q_HEADS, HEAD_DIM).astype(jnp.float32), cos_t, sin_t)
    queries = queries.astype(jnp.bfloat16)
    key_new = apply_rope(key_new.reshape(n_seqs, KV_HEADS, HEAD_DIM).astype(jnp.float32), cos_t, sin_t)
    key_new = key_new.astype(jnp.bfloat16)
    value_new = value_new.reshape(n_seqs, KV_HEADS, HEAD_DIM)
    slot_hit = (jnp.arange(CACHE_LEN)[None, :] == positions[:, None])[:, :, None, None]
    k_full = jnp.where(slot_hit, key_new[:, None], k_cache)
    v_full = jnp.where(slot_hit, value_new[:, None], v_cache)
    scale = 1.0 / math.sqrt(HEAD_DIM)

    def one_seq(seq_items):
        q_seq, k_seq, v_seq, pos_seq = seq_items
        q_grp = q_seq.reshape(KV_HEADS, group_size, HEAD_DIM).astype(jnp.float32)
        scores = jnp.einsum('kgd,skd->kgs', q_grp, k_seq.astype(jnp.float32)) * scale
        valid = jnp.arange(CACHE_LEN) <= pos_seq
        scores = jnp.where(valid[None, None, :], scores, -jnp.inf)
        attn_prob = jax.nn.softmax(scores, axis=-1).astype(jnp.bfloat16)
        attn_seq = jnp.einsum('kgs,skd->kgd', attn_prob.astype(jnp.float32), v_seq.astype(jnp.float32))
        return attn_seq.astype(jnp.bfloat16).reshape(Q_HEADS * HEAD_DIM)

    attn_out = lax.map(one_seq, (queries, k_full, v_full, positions))
    y_full = jnp.dot(attn_out, w_out, preferred_element_type=jnp.float32)
    resid_mid = (resid_in.astype(jnp.float32) + y_full).astype(jnp.bfloat16)
    normed_mlp = rms_norm(resid_mid, gain_mlp)
    gate_proj = jnp.dot(normed_mlp, w_gate, preferred_element_type=jnp.float32).astype(jnp.bfloat16)
    up_proj = jnp.dot(normed_mlp, w_up, preferred_element_type=jnp.float32).astype(jnp.bfloat16)
    hidden = (jax.nn.silu(gate_proj.astype(jnp.float32)) * up_proj.astype(jnp.float32)).astype(jnp.bfloat16)
    z_full = jnp.dot(hidden, w_down, preferred_element_type=jnp.float32)
    resid_out = (resid_mid.astype(jnp.float32) + z_full).astype(jnp.bfloat16)
    return resid_out, k_full, v_full
```

```python
import functools
import math
import jax
import jax.numpy as jnp
from jax import lax
from jax.experimental import pallas as pl
from jax.experimental.pallas import tpu as pltpu
from jax.sharding import PartitionSpec as P

EPS = 1e-5
ROPE_THETA = 500000.0
ROPE_FACTOR = 8.0
LOW_FACTOR = 1.0
HIGH_FACTOR = 4.0
ORIG_CTX = 8192.0

MESH = pl.DeviceIdType.MESH
BLK = 512
SLOTS = 11
LAG_D, LAG_1, LAG_2 = 3, 7, 11
GLAG_2, GLAG_3 = 3, 5
ZLAGS = (1, 3, 5, 7, 9, 11)


def rms_norm(rows_in, gain):
    rows_f = rows_in.astype(jnp.float32)
    mean_sq = jnp.mean(rows_f * rows_f, axis=-1, keepdims=True)
    return (rows_f * lax.rsqrt(mean_sq + EPS) * gain.astype(jnp.float32)).astype(jnp.bfloat16)


def rope_tables(positions, head_dim):
    half_dim = head_dim // 2
    exponents = jnp.arange(half_dim, dtype=jnp.float32) * (2.0 / head_dim)
    inv_freq = 1.0 / jnp.power(ROPE_THETA, exponents)
    wavelen = (2.0 * math.pi) / inv_freq
    smooth = (ORIG_CTX / wavelen - LOW_FACTOR) / (HIGH_FACTOR - LOW_FACTOR)
    blended = (1.0 - smooth) * inv_freq / ROPE_FACTOR + smooth * inv_freq
    inv_freq = jnp.where(wavelen < ORIG_CTX / HIGH_FACTOR, inv_freq,
                         jnp.where(wavelen > ORIG_CTX / LOW_FACTOR, inv_freq / ROPE_FACTOR, blended))
    angles = positions.astype(jnp.float32)[:, None] * inv_freq[None, :]
    return jnp.cos(angles), jnp.sin(angles)


def apply_rope(vectors, cos_t, sin_t):
    half_dim = vectors.shape[-1] // 2
    lower_half = vectors[..., :half_dim]
    upper_half = vectors[..., half_dim:]
    cos_b = cos_t[:, None, :]
    sin_b = sin_t[:, None, :]
    return jnp.concatenate([lower_half * cos_b - upper_half * sin_b,
                            upper_half * cos_b + lower_half * sin_b], axis=-1)


def attention_block(resid_in, positions, k_cache, v_cache, gain_attn, w_query, w_key, w_value):
    n_seqs = resid_in.shape[0]
    cache_len = k_cache.shape[1]
    kv_heads = k_cache.shape[2]
    head_dim = k_cache.shape[3]
    group_size = w_query.shape[1] // (kv_heads * head_dim)
    normed = rms_norm(resid_in, gain_attn)
    queries = jnp.dot(normed, w_query, preferred_element_type=jnp.float32).astype(jnp.bfloat16)
    key_new = jnp.dot(normed, w_key, preferred_element_type=jnp.float32).astype(jnp.bfloat16)
    value_new = jnp.dot(normed, w_value, preferred_element_type=jnp.float32).astype(jnp.bfloat16)
    cos_t, sin_t = rope_tables(positions, head_dim)
    queries = apply_rope(queries.reshape(n_seqs, kv_heads * group_size, head_dim).astype(jnp.float32), cos_t, sin_t)
    queries = queries.astype(jnp.bfloat16).reshape(n_seqs, kv_heads, group_size, head_dim)
    key_new = apply_rope(key_new.reshape(n_seqs, kv_heads, head_dim).astype(jnp.float32), cos_t, sin_t)
    key_new = key_new.astype(jnp.bfloat16)
    value_new = value_new.reshape(n_seqs, kv_heads, head_dim)
    slot_iota = lax.broadcasted_iota(jnp.int32, (n_seqs, cache_len), 1)
    slot_hit = (slot_iota == positions[:, None])[:, :, None, None]
    k_full = jnp.where(slot_hit, key_new[:, None], k_cache)
    v_full = jnp.where(slot_hit, value_new[:, None], v_cache)
    scores = jnp.einsum('bkgd,bskd->bkgs', queries, k_full, preferred_element_type=jnp.float32)
    scores = scores * (1.0 / math.sqrt(head_dim))
    valid = (slot_iota <= positions[:, None])[:, None, None, :]
    scores = jnp.where(valid, scores, -jnp.inf)
    attn_prob = jax.nn.softmax(scores, axis=-1).astype(jnp.bfloat16)
    attn_out = jnp.einsum('bkgs,bskd->bkgd', attn_prob, v_full, preferred_element_type=jnp.float32)
    attn_out = attn_out.astype(jnp.bfloat16).reshape(n_seqs, kv_heads * group_size * head_dim)
    return attn_out, k_full, v_full


def mlp_kernel(dims, o_ref, resid_ref, gain_ref, wo_ref, wg_ref, wu_ref, wd_ref, out_ref,
               ring, ybuf, r_d, r_1, r_2, hbuf, acc_g, acc_u, hidden, x_own, rows_own,
               w_sem, l_sem, snd, rcv):
    n_ch, n_fb, rows = dims
    me = lax.axis_index('tp')
    core = lax.rem(me, 2)
    chip = me // 2
    apair = chip // 2
    bpair = lax.rem((chip + 1) // 2, 2)
    chip_a = chip + 1 - 2 * lax.rem(chip, 2)
    chip_b = 3 - chip
    hi = bpair + core * (apair - bpair)
    lo = apair + core * (bpair - apair)
    first = 2 * (chip_a + core * (chip_b - chip_a)) + core
    second = 2 * (chip_b + core * (chip_a - chip_b)) + core
    mate = 2 * chip + 1 - core
    half = 4 * core
    own = half + 2 * hi + lo

    def remote(stage, u, src, dst, dev):
        return pltpu.make_async_remote_copy(src_ref=src, dst_ref=dst, send_sem=snd.at[stage, u], recv_sem=rcv.at[stage, u],
                                            device_id={'tp': dev}, device_id_type=MESH)

    def s_d(u):
        return remote(0, u, ybuf.at[u, pl.ds(4 - half, 4)], r_d.at[u], mate)

    def s_1(u):
        return remote(1, u, ybuf.at[u, pl.ds(half + 2 - 2 * hi, 2)], r_1.at[u], first)

    def s_2(u):
        return remote(2, u, ybuf.at[u, half + 2 * hi + 1 - lo], r_2.at[u], second)

    def g_1(u):
        return remote(3, u, hbuf.at[u, own], hbuf.at[u, own], second)

    def g_2(u):
        return remote(4, u, hbuf.at[u, pl.ds(half + 2 * hi, 2)], hbuf.at[u, pl.ds(half + 2 * hi, 2)], first)

    def g_3(u):
        return remote(5, u, hbuf.at[u, pl.ds(half, 4)], hbuf.at[u, pl.ds(half, 4)], mate)

    def load_out(b, slot, idx):
        return pltpu.make_async_copy(wo_ref.at[:, pl.ds(pl.multiple_of(b * BLK, BLK), BLK)], ring.at[slot, idx], w_sem.at[slot])

    def issue(load):
        slot = lax.rem(load, SLOTS)
        seq = load - 2

        def rows_of(w_ref, k):
            for b in range(n_fb):
                pltpu.make_async_copy(w_ref.at[pl.ds(pl.multiple_of(k * BLK, BLK), BLK), pl.ds(b * BLK, BLK)],
                                      ring.at[slot, b], w_sem.at[slot]).start()

        @pl.when((seq < 2 * n_ch) & (lax.rem(seq, 2) == 0))
        def _():
            rows_of(wg_ref, seq // 2)

        @pl.when((seq < 2 * n_ch) & (lax.rem(seq, 2) == 1))
        def _():
            rows_of(wu_ref, seq // 2)

        @pl.when((seq >= 2 * n_ch) & (seq < 3 * n_ch))
        def _():
            for b in range(n_fb):
                pltpu.make_async_copy(wd_ref.at[pl.ds(b * BLK, BLK), pl.ds(pl.multiple_of((seq - 2 * n_ch) * BLK, BLK), BLK)],
                                      ring.at[slot, b], w_sem.at[slot]).start()

    def wait_load(load):
        slot = lax.rem(load, SLOTS)
        pltpu.make_async_copy(ring.at[slot], ring.at[slot], w_sem.at[slot]).wait()
        return slot

    for b in range(n_fb):
        load_out(b, 0, b).start()
    for b in range(n_fb, n_ch):
        load_out(b, 1, b - n_fb).start()
    row_copy = pltpu.make_async_copy(resid_ref.at[pl.ds(pl.multiple_of(own * rows, rows), rows)], rows_own, l_sem)
    row_copy.start()

    def first_loads(i, c):
        issue(i)
        return c
    lax.fori_loop(2, SLOTS, first_loads, 0)

    barrier = pltpu.get_barrier_semaphore()
    for dev in (mate, first, second):
        pl.semaphore_signal(barrier, inc=1, device_id={'tp': dev}, device_id_type=MESH)
    pl.semaphore_wait(barrier, 3)

    def at(t, lag, fn):
        @pl.when((t >= lag) & (t < lag + n_ch))
        def _():
            fn(t - lag)

    def after_d(u):
        s_d(u).wait_recv()
        ybuf[u, pl.ds(half, 4)] += r_d[u]
        s_1(u).start()

    def after_1(u):
        s_1(u).wait_recv()
        ybuf[u, pl.ds(half + 2 * hi, 2)] += r_1[u]
        s_2(u).start()

    wait_load(0)
    pltpu.make_async_copy(ring.at[1, pl.ds(0, n_ch - n_fb)], ring.at[1, pl.ds(0, n_ch - n_fb)], w_sem.at[1]).wait()

    def step_y(t, c):
        def make(u):
            blk = ring[u // n_fb, lax.rem(u, n_fb)]
            y = jnp.dot(o_ref[...], blk, preferred_element_type=jnp.float32)
            ybuf[u] = y.reshape(8, rows, BLK)
            s_d(u).start()
        at(t, 0, make)

        @pl.when(t == n_ch)
        def _():
            issue(SLOTS)
            issue(SLOTS + 1)
        at(t, LAG_D, after_d)
        at(t, LAG_1, after_1)

        def done(u):
            s_2(u).wait_recv()
            x_own[u] = ybuf[u, own] + r_2[u]
        at(t, LAG_2, done)
        return c
    lax.fori_loop(0, n_ch + LAG_2, step_y, 0)

    def drain(u, c):
        s_d(u).wait_send()
        s_1(u).wait_send()
        s_2(u).wait_send()
        return c
    lax.fori_loop(0, n_ch, drain, 0)

    row_copy.wait()
    total = jnp.zeros((rows, 1), jnp.float32)
    for u in range(n_ch):
        x1 = (rows_own[:, u * BLK:(u + 1) * BLK].astype(jnp.float32) + x_own[u]).astype(jnp.bfloat16).astype(jnp.float32)
        x_own[u] = x1
        total += jnp.sum(x1 * x1, axis=-1, keepdims=True)
    inv = lax.rsqrt(total * (1.0 / (n_ch * BLK)) + EPS)
    for u in range(n_ch):
        gain = gain_ref[:, u * BLK:(u + 1) * BLK].astype(jnp.float32)
        hbuf[u, own] = (x_own[u] * inv * gain).astype(jnp.bfloat16).astype(jnp.float32)
        g_1(u).start()

    acc_g[...] = jnp.zeros_like(acc_g)
    acc_u[...] = jnp.zeros_like(acc_u)

    def step_g(t, c):
        def fwd_1(u):
            g_1(u).wait_recv()
            g_2(u).start()
        at(t, 0, fwd_1)

        def fwd_2(u):
            g_2(u).wait_recv()
            g_3(u).start()
        at(t, GLAG_2, fwd_2)

        def compute(u):
            g_3(u).wait_recv()
            h_k = hbuf[u].reshape(8 * rows, BLK).astype(jnp.bfloat16)
            for which, acc in ((0, acc_g), (1, acc_u)):
                load = 2 + 2 * u + which
                slot = wait_load(load)
                for b in range(n_fb):
                    acc[b] += jnp.dot(h_k, ring[slot, b], preferred_element_type=jnp.float32)
                issue(load + SLOTS)
        at(t, GLAG_3, compute)
        return c
    lax.fori_loop(0, n_ch + GLAG_3, step_g, 0)

    def drain_g(u, c):
        g_1(u).wait_send()
        g_2(u).wait_send()
        g_3(u).wait_send()
        return c
    lax.fori_loop(0, n_ch, drain_g, 0)

    for b in range(n_fb):
        gate = acc_g[b].astype(jnp.bfloat16).astype(jnp.float32)
        up = acc_u[b].astype(jnp.bfloat16).astype(jnp.float32)
        hidden[:, b * BLK:(b + 1) * BLK] = (gate * jax.nn.sigmoid(gate) * up).astype(jnp.bfloat16)

    def step_z(t, c):
        def make(u):
            slot = wait_load(2 + 2 * n_ch + u)
            z = jnp.dot(hidden[...], ring[slot].reshape(n_fb * BLK, BLK), preferred_element_type=jnp.float32)
            ybuf[u] = z.reshape(8, rows, BLK)
            s_d(u).start()
        at(t, 0, make)
        at(t, ZLAGS[0], after_d)
        at(t, ZLAGS[1], after_1)

        def done(u):
            s_2(u).wait_recv()
            hbuf[u, own] = (x_own[u] + (ybuf[u, own] + r_2[u])).astype(jnp.bfloat16).astype(jnp.float32)
            g_1(u).start()
        at(t, ZLAGS[2], done)

        def fwd_1(u):
            g_1(u).wait_recv()
            g_2(u).start()
        at(t, ZLAGS[3], fwd_1)

        def fwd_2(u):
            g_2(u).wait_recv()
            g_3(u).start()
        at(t, ZLAGS[4], fwd_2)

        def write(u):
            g_3(u).wait_recv()
            out_ref[:, pl.ds(pl.multiple_of(u * BLK, BLK), BLK)] = hbuf[u].reshape(8 * rows, BLK).astype(jnp.bfloat16)
        at(t, ZLAGS[5], write)
        return c
    lax.fori_loop(0, n_ch + ZLAGS[5], step_z, 0)
    lax.fori_loop(0, n_ch, drain, 0)
    lax.fori_loop(0, n_ch, drain_g, 0)


def mlp_part(attn_out, resid_in, gain_mlp, w_out, w_gate, w_up, w_down):
    n_seqs, model = resid_in.shape
    ffn = w_gate.shape[1]
    n_ch, n_fb, rows = model // BLK, ffn // BLK, n_seqs // 8
    f32, bf16 = jnp.float32, jnp.bfloat16
    any_spec = pl.BlockSpec(memory_space=pltpu.HBM)
    vmem_spec = pl.BlockSpec(memory_space=pltpu.VMEM)
    return pl.pallas_call(
        functools.partial(mlp_kernel, (n_ch, n_fb, rows)),
        out_shape=jax.ShapeDtypeStruct((n_seqs, model), bf16),
        in_specs=[vmem_spec, any_spec, vmem_spec, any_spec, any_spec, any_spec, any_spec],
        out_specs=vmem_spec,
        scratch_shapes=[
            pltpu.VMEM((SLOTS, n_fb, BLK, BLK), bf16),
            pltpu.VMEM((n_ch, 8, rows, BLK), f32),
            pltpu.VMEM((n_ch, 4, rows, BLK), f32),
            pltpu.VMEM((n_ch, 2, rows, BLK), f32),
            pltpu.VMEM((n_ch, rows, BLK), f32),
            pltpu.VMEM((n_ch, 8, rows, BLK), f32),
            pltpu.VMEM((n_fb, n_seqs, BLK), f32),
            pltpu.VMEM((n_fb, n_seqs, BLK), f32),
            pltpu.VMEM((n_seqs, ffn), bf16),
            pltpu.VMEM((n_ch, rows, BLK), f32),
            pltpu.VMEM((rows, model), bf16),
            pltpu.SemaphoreType.DMA((SLOTS,)),
            pltpu.SemaphoreType.DMA,
            pltpu.SemaphoreType.DMA((6, n_ch)),
            pltpu.SemaphoreType.DMA((6, n_ch)),
        ],
        compiler_params=pltpu.CompilerParams(collective_id=0, has_side_effects=True, vmem_limit_bytes=66_900_000),
        cost_estimate=pl.CostEstimate(flops=6 * n_seqs * model * ffn, bytes_accessed=6 * model * ffn, transcendentals=0),
        name='out_mlp',
    )(attn_out, resid_in, gain_mlp.reshape(1, model), w_out, w_gate, w_up, w_down)


def solution(mesh):
    def layer_local(resid_in, positions, k_cache, v_cache, gain_attn, w_query, w_key, w_value,
                    w_out, gain_mlp, w_gate, w_up, w_down):
        attn_out, k_full, v_full = attention_block(resid_in, positions, k_cache, v_cache,
                                                   gain_attn, w_query, w_key, w_value)
        resid_out = mlp_part(attn_out, resid_in, gain_mlp, w_out, w_gate, w_up, w_down)
        return resid_out, k_full, v_full

    row_spec = P('dp', None)
    cache_spec = P('dp', None, 'tp', None)
    col_spec = P(None, 'tp')
    split_rows = P('tp', None)
    return jax.shard_map(layer_local, mesh=mesh,
                         in_specs=(row_spec, P('dp'), cache_spec, cache_spec, P(), col_spec, col_spec,
                                   col_spec, split_rows, P(), col_spec, col_spec, split_rows),
                         out_specs=(row_spec, cache_spec, cache_spec), check_vma=False)
```

```python
import functools
import math
import jax
import jax.numpy as jnp
import numpy as np
from jax import lax
from jax.experimental import pallas as pl
from jax.experimental.pallas import tpu as pltpu
from jax.sharding import PartitionSpec as P

EPS = 1e-5
ROPE_THETA = 500000.0
ROPE_FACTOR = 8.0
LOW_FACTOR = 1.0
HIGH_FACTOR = 4.0
ORIG_CTX = 8192.0

MESH = pl.DeviceIdType.MESH
BLK = 512
SLOTS = 11
SB = 8
UNROLL = 4
QCH = 5
LAG_D, LAG_1, LAG_2 = 3, 7, 11
GLAG_2, GLAG_3 = 3, 5
ZLAGS = (1, 3, 5, 7, 9, 11)


def rope_freqs(head_dim):
    exponents = np.arange(head_dim // 2) * (2.0 / head_dim)
    inv_freq = 1.0 / np.power(ROPE_THETA, exponents)
    wavelen = (2.0 * math.pi) / inv_freq
    smooth = (ORIG_CTX / wavelen - LOW_FACTOR) / (HIGH_FACTOR - LOW_FACTOR)
    blended = (1.0 - smooth) * inv_freq / ROPE_FACTOR + smooth * inv_freq
    inv_freq = np.where(wavelen < ORIG_CTX / HIGH_FACTOR, inv_freq,
                        np.where(wavelen > ORIG_CTX / LOW_FACTOR, inv_freq / ROPE_FACTOR, blended))
    return np.concatenate([inv_freq, inv_freq])[None].astype(np.float32)


def attn_kernel(pos_s, resid_ref, gain_ref, pos_ref, freq_ref, wq_ref, wk_ref, wv_ref, kc_ref, vc_ref,
                out_ref, ko_ref, vo_ref, wq, wk, wv, kbuf, vbuf, normed, q_rot, k_rot, v_new, pos_b, o_buf,
                q_sem, k_sem, v_sem, ko_sem, vo_sem):
    f32, bf16 = jnp.float32, jnp.bfloat16
    n_seqs, model = resid_ref.shape
    cache_len, dim = kbuf.shape[1], kbuf.shape[2]
    heads = wq.shape[1] // dim
    n_blk = n_seqs // SB
    kc = model // QCH

    def w_copies(i):
        sl = pl.ds(i * kc, kc)
        return [pltpu.make_async_copy(src.at[sl], dst.at[sl], q_sem.at[i, j])
                for j, (src, dst) in enumerate(((wq_ref, wq), (wk_ref, wk), (wv_ref, wv)))]

    def seqs(i):
        return pl.ds(pl.multiple_of(i * SB, SB), SB)

    def k_in(i):
        return pltpu.make_async_copy(kc_ref.at[seqs(i)], kbuf.at[seqs(i)], k_sem.at[i])

    def v_in(i):
        return pltpu.make_async_copy(vc_ref.at[seqs(i)], vbuf.at[seqs(i)], v_sem.at[i])

    def k_out(i):
        return pltpu.make_async_copy(kbuf.at[seqs(i)], ko_ref.at[seqs(i)], ko_sem.at[i])

    def v_out(i):
        return pltpu.make_async_copy(vbuf.at[seqs(i)], vo_ref.at[seqs(i)], vo_sem.at[i])

    for i in range(QCH):
        for c in w_copies(i):
            c.start()
    for i in range(n_blk):
        k_in(i).start()
        v_in(i).start()

    row_i = lax.broadcasted_iota(jnp.int32, (n_seqs, n_seqs), 0)
    col_i = lax.broadcasted_iota(jnp.int32, (n_seqs, n_seqs), 1)
    pos_f = pos_ref[...].astype(f32)
    pos_col = jnp.sum(jnp.where(row_i == col_i, pos_f, 0.0), axis=1, keepdims=True)
    pos_b[...] = jnp.broadcast_to(pos_col, pos_b.shape)
    angles = pos_b[...] * freq_ref[...]
    cos_t = jnp.cos(angles)
    lane = lax.broadcasted_iota(jnp.int32, angles.shape, 1)
    sin_t = jnp.sin(angles)
    sin_t = jnp.where(lane < dim // 2, -sin_t, sin_t)

    total = jnp.zeros((n_seqs, 1), f32)
    for i in range(QCH):
        x = resid_ref[:, i * kc:(i + 1) * kc].astype(f32)
        total += jnp.sum(x * x, axis=-1, keepdims=True)
    inv = lax.rsqrt(total * (1.0 / model) + EPS)
    for i in range(QCH):
        sl = slice(i * kc, (i + 1) * kc)
        normed[:, sl] = (resid_ref[:, sl].astype(f32) * inv * gain_ref[:, sl].astype(f32)).astype(bf16)

    q = k = v = None
    for i in range(QCH):
        for c in w_copies(i):
            c.wait()
        sl = slice(i * kc, (i + 1) * kc)
        h = normed[:, sl]
        parts = [jnp.dot(h, w[sl, :], preferred_element_type=f32) for w in (wq, wk, wv)]
        q, k, v = parts if q is None else [x + y for x, y in zip((q, k, v), parts)]

    def rope(x):
        x = x.astype(bf16).astype(f32)
        return (x * cos_t + pltpu.roll(x, dim // 2, 1) * sin_t).astype(bf16).astype(f32)

    for j in range(heads):
        q_rot[j] = rope(q[:, j * dim:(j + 1) * dim])
    k_rot[...] = rope(k)
    v_new[...] = v.astype(bf16).astype(f32)

    rows, cols = heads * SB, SB * cache_len
    r_i = lax.broadcasted_iota(jnp.int32, (rows, cols), 0)
    c_i = lax.broadcasted_iota(jnp.int32, (rows, cols), 1)
    slot_of = jnp.where(lax.rem(r_i, SB) == c_i // cache_len, lax.rem(c_i, cache_len), 2 * cache_len).astype(f32)
    slot_row = lax.broadcasted_iota(jnp.int32, (cache_len, dim), 0)
    scale = 1.0 / math.sqrt(dim)

    def block(i):
        k_in(i).wait()
        v_in(i).wait()
        for s in range(SB):
            n = i * SB + s
            hit = slot_row == pos_s[n]
            kbuf[n] = jnp.where(hit, k_rot[pl.ds(n, 1), :], kbuf[n].astype(f32)).astype(bf16)
            vbuf[n] = jnp.where(hit, v_new[pl.ds(n, 1), :], vbuf[n].astype(f32)).astype(bf16)
        k_out(i).start()
        v_out(i).start()
        q_b = jnp.concatenate([q_rot[j, seqs(i), :] for j in range(heads)], axis=0).astype(bf16)
        k_b = kbuf[seqs(i)].reshape(cols, dim)
        v_b = vbuf[seqs(i)].reshape(cols, dim)
        sc = lax.dot_general(q_b, k_b, (((1,), (1,)), ((), ())), preferred_element_type=f32) * scale
        p_b = jnp.concatenate([pos_b[seqs(i), :]] * heads, axis=0)
        p_b = jnp.concatenate([p_b] * SB, axis=1)
        sc = jnp.where(slot_of <= p_b, sc, -jnp.inf)
        ex = jnp.exp(sc - jnp.max(sc, axis=-1, keepdims=True))
        prob = (ex * (1.0 / jnp.sum(ex, axis=-1, keepdims=True))).astype(bf16)
        o = jnp.dot(prob, v_b, preferred_element_type=f32)
        for j in range(heads):
            o_buf[seqs(i), j * dim:(j + 1) * dim] = o[j * SB:(j + 1) * SB]

    def step(g, c):
        for r in range(UNROLL):
            block(g * UNROLL + r)
        return c
    lax.fori_loop(0, n_blk // UNROLL, step, 0)
    out_ref[...] = o_buf[...].astype(bf16)

    def finish(i, c):
        k_out(i).wait()
        v_out(i).wait()
        return c
    lax.fori_loop(0, n_blk, finish, 0)


def attention_part(resid_in, positions, k_cache, v_cache, gain_attn, w_query, w_key, w_value):
    n_seqs, model = resid_in.shape
    cache_len, kv_heads, dim = k_cache.shape[1:]
    q_width = w_query.shape[1]
    f32, bf16 = jnp.float32, jnp.bfloat16
    cache_flat = (n_seqs, cache_len * kv_heads, dim)
    hbm = pl.BlockSpec(memory_space=pltpu.HBM)
    vmem = pl.BlockSpec(memory_space=pltpu.VMEM)
    smem = pl.BlockSpec(memory_space=pltpu.SMEM)
    n_blk = n_seqs // SB
    out, k_full, v_full = pl.pallas_call(
        attn_kernel,
        out_shape=(jax.ShapeDtypeStruct((n_seqs, q_width), bf16), jax.ShapeDtypeStruct(cache_flat, bf16),
                   jax.ShapeDtypeStruct(cache_flat, bf16)),
        in_specs=[smem, vmem, vmem, vmem, vmem, hbm, hbm, hbm, hbm, hbm],
        out_specs=(vmem, hbm, hbm),
        scratch_shapes=[
            pltpu.VMEM(w_query.shape, bf16), pltpu.VMEM(w_key.shape, bf16), pltpu.VMEM(w_value.shape, bf16),
            pltpu.VMEM(cache_flat, bf16), pltpu.VMEM(cache_flat, bf16),
            pltpu.VMEM((n_seqs, model), bf16), pltpu.VMEM((q_width // dim, n_seqs, dim), f32),
            pltpu.VMEM((n_seqs, dim), f32), pltpu.VMEM((n_seqs, dim), f32), pltpu.VMEM((n_seqs, dim), f32),
            pltpu.VMEM((n_seqs, q_width), f32),
            pltpu.SemaphoreType.DMA((QCH, 3)),
            pltpu.SemaphoreType.DMA((n_blk,)), pltpu.SemaphoreType.DMA((n_blk,)),
            pltpu.SemaphoreType.DMA((n_blk,)), pltpu.SemaphoreType.DMA((n_blk,)),
        ],
        compiler_params=pltpu.CompilerParams(vmem_limit_bytes=60_000_000),
        cost_estimate=pl.CostEstimate(flops=2 * n_seqs * model * q_width, bytes_accessed=30_000_000, transcendentals=0),
        name='attn',
    )(positions, resid_in, gain_attn.reshape(1, model), positions.reshape(1, n_seqs), rope_freqs(dim),
      w_query, w_key, w_value, k_cache.reshape(cache_flat), v_cache.reshape(cache_flat))
    return out, k_full.reshape(k_cache.shape), v_full.reshape(v_cache.shape)


def mlp_kernel(dims, o_ref, resid_ref, gain_ref, wo_ref, wg_ref, wu_ref, wd_ref, out_ref,
               ring, ybuf, r_d, r_1, r_2, hbuf, acc_g, acc_u, hidden, x_own, rows_own,
               w_sem, l_sem, snd, rcv):
    n_ch, n_fb, rows = dims
    me = lax.axis_index('tp')
    core = lax.rem(me, 2)
    chip = me // 2
    apair = chip // 2
    bpair = lax.rem((chip + 1) // 2, 2)
    chip_a = chip + 1 - 2 * lax.rem(chip, 2)
    chip_b = 3 - chip
    hi = bpair + core * (apair - bpair)
    lo = apair + core * (bpair - apair)
    first = 2 * (chip_a + core * (chip_b - chip_a)) + core
    second = 2 * (chip_b + core * (chip_a - chip_b)) + core
    mate = 2 * chip + 1 - core
    half = 4 * core
    own = half + 2 * hi + lo

    def remote(stage, u, src, dst, dev):
        return pltpu.make_async_remote_copy(src_ref=src, dst_ref=dst, send_sem=snd.at[stage, u], recv_sem=rcv.at[stage, u],
                                            device_id={'tp': dev}, device_id_type=MESH)

    def s_d(u):
        return remote(0, u, ybuf.at[u, pl.ds(4 - half, 4)], r_d.at[u], mate)

    def s_1(u):
        return remote(1, u, ybuf.at[u, pl.ds(half + 2 - 2 * hi, 2)], r_1.at[u], first)

    def s_2(u):
        return remote(2, u, ybuf.at[u, half + 2 * hi + 1 - lo], r_2.at[u], second)

    def g_1(u):
        return remote(3, u, hbuf.at[u, own], hbuf.at[u, own], second)

    def g_2(u):
        return remote(4, u, hbuf.at[u, pl.ds(half + 2 * hi, 2)], hbuf.at[u, pl.ds(half + 2 * hi, 2)], first)

    def g_3(u):
        return remote(5, u, hbuf.at[u, pl.ds(half, 4)], hbuf.at[u, pl.ds(half, 4)], mate)

    def load_out(b, slot, idx):
        return pltpu.make_async_copy(wo_ref.at[:, pl.ds(pl.multiple_of(b * BLK, BLK), BLK)], ring.at[slot, idx], w_sem.at[slot])

    def issue(load):
        slot = lax.rem(load, SLOTS)
        seq = load - 2

        def rows_of(w_ref, k):
            for b in range(n_fb):
                pltpu.make_async_copy(w_ref.at[pl.ds(pl.multiple_of(k * BLK, BLK), BLK), pl.ds(b * BLK, BLK)],
                                      ring.at[slot, b], w_sem.at[slot]).start()

        @pl.when((seq < 2 * n_ch) & (lax.rem(seq, 2) == 0))
        def _():
            rows_of(wg_ref, seq // 2)

        @pl.when((seq < 2 * n_ch) & (lax.rem(seq, 2) == 1))
        def _():
            rows_of(wu_ref, seq // 2)

        @pl.when((seq >= 2 * n_ch) & (seq < 3 * n_ch))
        def _():
            for b in range(n_fb):
                pltpu.make_async_copy(wd_ref.at[pl.ds(b * BLK, BLK), pl.ds(pl.multiple_of((seq - 2 * n_ch) * BLK, BLK), BLK)],
                                      ring.at[slot, b], w_sem.at[slot]).start()

    def wait_load(load):
        slot = lax.rem(load, SLOTS)
        pltpu.make_async_copy(ring.at[slot], ring.at[slot], w_sem.at[slot]).wait()
        return slot

    for b in range(n_fb):
        load_out(b, 0, b).start()
    for b in range(n_fb, n_ch):
        load_out(b, 1, b - n_fb).start()
    row_copy = pltpu.make_async_copy(resid_ref.at[pl.ds(pl.multiple_of(own * rows, rows), rows)], rows_own, l_sem)
    row_copy.start()

    def first_loads(i, c):
        issue(i)
        return c
    lax.fori_loop(2, SLOTS, first_loads, 0)

    barrier = pltpu.get_barrier_semaphore()
    for dev in (mate, first, second):
        pl.semaphore_signal(barrier, inc=1, device_id={'tp': dev}, device_id_type=MESH)
    pl.semaphore_wait(barrier, 3)

    def at(t, lag, fn):
        @pl.when((t >= lag) & (t < lag + n_ch))
        def _():
            fn(t - lag)

    def after_d(u):
        s_d(u).wait_recv()
        ybuf[u, pl.ds(half, 4)] += r_d[u]
        s_1(u).start()

    def after_1(u):
        s_1(u).wait_recv()
        ybuf[u, pl.ds(half + 2 * hi, 2)] += r_1[u]
        s_2(u).start()

    wait_load(0)
    pltpu.make_async_copy(ring.at[1, pl.ds(0, n_ch - n_fb)], ring.at[1, pl.ds(0, n_ch - n_fb)], w_sem.at[1]).wait()

    def step_y(t, c):
        def make(u):
            blk = ring[u // n_fb, lax.rem(u, n_fb)]
            y = jnp.dot(o_ref[...], blk, preferred_element_type=jnp.float32)
            ybuf[u] = y.reshape(8, rows, BLK)
            s_d(u).start()
        at(t, 0, make)

        @pl.when(t == n_ch)
        def _():
            issue(SLOTS)
            issue(SLOTS + 1)
        at(t, LAG_D, after_d)
        at(t, LAG_1, after_1)

        def done(u):
            s_2(u).wait_recv()
            x_own[u] = ybuf[u, own] + r_2[u]
        at(t, LAG_2, done)
        return c
    lax.fori_loop(0, n_ch + LAG_2, step_y, 0)

    def drain(u, c):
        s_d(u).wait_send()
        s_1(u).wait_send()
        s_2(u).wait_send()
        return c
    lax.fori_loop(0, n_ch, drain, 0)

    row_copy.wait()
    total = jnp.zeros((rows, 1), jnp.float32)
    for u in range(n_ch):
        x1 = (rows_own[:, u * BLK:(u + 1) * BLK].astype(jnp.float32) + x_own[u]).astype(jnp.bfloat16).astype(jnp.float32)
        x_own[u] = x1
        total += jnp.sum(x1 * x1, axis=-1, keepdims=True)
    inv = lax.rsqrt(total * (1.0 / (n_ch * BLK)) + EPS)
    for u in range(n_ch):
        gain = gain_ref[:, u * BLK:(u + 1) * BLK].astype(jnp.float32)
        hbuf[u, own] = (x_own[u] * inv * gain).astype(jnp.bfloat16).astype(jnp.float32)
        g_1(u).start()

    acc_g[...] = jnp.zeros_like(acc_g)
    acc_u[...] = jnp.zeros_like(acc_u)

    def step_g(t, c):
        def fwd_1(u):
            g_1(u).wait_recv()
            g_2(u).start()
        at(t, 0, fwd_1)

        def fwd_2(u):
            g_2(u).wait_recv()
            g_3(u).start()
        at(t, GLAG_2, fwd_2)

        def compute(u):
            g_3(u).wait_recv()
            h_k = hbuf[u].reshape(8 * rows, BLK).astype(jnp.bfloat16)
            for which, acc in ((0, acc_g), (1, acc_u)):
                load = 2 + 2 * u + which
                slot = wait_load(load)
                for b in range(n_fb):
                    acc[b] += jnp.dot(h_k, ring[slot, b], preferred_element_type=jnp.float32)
                issue(load + SLOTS)
        at(t, GLAG_3, compute)
        return c
    lax.fori_loop(0, n_ch + GLAG_3, step_g, 0)

    def drain_g(u, c):
        g_1(u).wait_send()
        g_2(u).wait_send()
        g_3(u).wait_send()
        return c
    lax.fori_loop(0, n_ch, drain_g, 0)

    for b in range(n_fb):
        gate = acc_g[b].astype(jnp.bfloat16).astype(jnp.float32)
        up = acc_u[b].astype(jnp.bfloat16).astype(jnp.float32)
        hidden[:, b * BLK:(b + 1) * BLK] = (gate * jax.nn.sigmoid(gate) * up).astype(jnp.bfloat16)

    def step_z(t, c):
        def make(u):
            slot = wait_load(2 + 2 * n_ch + u)
            z = jnp.dot(hidden[...], ring[slot].reshape(n_fb * BLK, BLK), preferred_element_type=jnp.float32)
            ybuf[u] = z.reshape(8, rows, BLK)
            s_d(u).start()
        at(t, 0, make)
        at(t, ZLAGS[0], after_d)
        at(t, ZLAGS[1], after_1)

        def done(u):
            s_2(u).wait_recv()
            hbuf[u, own] = (x_own[u] + (ybuf[u, own] + r_2[u])).astype(jnp.bfloat16).astype(jnp.float32)
            g_1(u).start()
        at(t, ZLAGS[2], done)

        def fwd_1(u):
            g_1(u).wait_recv()
            g_2(u).start()
        at(t, ZLAGS[3], fwd_1)

        def fwd_2(u):
            g_2(u).wait_recv()
            g_3(u).start()
        at(t, ZLAGS[4], fwd_2)

        def write(u):
            g_3(u).wait_recv()
            out_ref[:, pl.ds(pl.multiple_of(u * BLK, BLK), BLK)] = hbuf[u].reshape(8 * rows, BLK).astype(jnp.bfloat16)
        at(t, ZLAGS[5], write)
        return c
    lax.fori_loop(0, n_ch + ZLAGS[5], step_z, 0)
    lax.fori_loop(0, n_ch, drain, 0)
    lax.fori_loop(0, n_ch, drain_g, 0)


def mlp_part(attn_out, resid_in, gain_mlp, w_out, w_gate, w_up, w_down):
    n_seqs, model = resid_in.shape
    ffn = w_gate.shape[1]
    n_ch, n_fb, rows = model // BLK, ffn // BLK, n_seqs // 8
    f32, bf16 = jnp.float32, jnp.bfloat16
    any_spec = pl.BlockSpec(memory_space=pltpu.HBM)
    vmem_spec = pl.BlockSpec(memory_space=pltpu.VMEM)
    return pl.pallas_call(
        functools.partial(mlp_kernel, (n_ch, n_fb, rows)),
        out_shape=jax.ShapeDtypeStruct((n_seqs, model), bf16),
        in_specs=[vmem_spec, any_spec, vmem_spec, any_spec, any_spec, any_spec, any_spec],
        out_specs=vmem_spec,
        scratch_shapes=[
            pltpu.VMEM((SLOTS, n_fb, BLK, BLK), bf16),
            pltpu.VMEM((n_ch, 8, rows, BLK), f32),
            pltpu.VMEM((n_ch, 4, rows, BLK), f32),
            pltpu.VMEM((n_ch, 2, rows, BLK), f32),
            pltpu.VMEM((n_ch, rows, BLK), f32),
            pltpu.VMEM((n_ch, 8, rows, BLK), f32),
            pltpu.VMEM((n_fb, n_seqs, BLK), f32),
            pltpu.VMEM((n_fb, n_seqs, BLK), f32),
            pltpu.VMEM((n_seqs, ffn), bf16),
            pltpu.VMEM((n_ch, rows, BLK), f32),
            pltpu.VMEM((rows, model), bf16),
            pltpu.SemaphoreType.DMA((SLOTS,)),
            pltpu.SemaphoreType.DMA,
            pltpu.SemaphoreType.DMA((6, n_ch)),
            pltpu.SemaphoreType.DMA((6, n_ch)),
        ],
        compiler_params=pltpu.CompilerParams(collective_id=0, has_side_effects=True, vmem_limit_bytes=66_900_000),
        cost_estimate=pl.CostEstimate(flops=6 * n_seqs * model * ffn, bytes_accessed=6 * model * ffn, transcendentals=0),
        name='out_mlp',
    )(attn_out, resid_in, gain_mlp.reshape(1, model), w_out, w_gate, w_up, w_down)


def solution(mesh):
    def layer_local(resid_in, positions, k_cache, v_cache, gain_attn, w_query, w_key, w_value,
                    w_out, gain_mlp, w_gate, w_up, w_down):
        attn_out, k_full, v_full = attention_part(resid_in, positions, k_cache, v_cache,
                                                  gain_attn, w_query, w_key, w_value)
        resid_out = mlp_part(attn_out, resid_in, gain_mlp, w_out, w_gate, w_up, w_down)
        return resid_out, k_full, v_full

    row_spec = P('dp', None)
    cache_spec = P('dp', None, 'tp', None)
    col_spec = P(None, 'tp')
    split_rows = P('tp', None)
    return jax.shard_map(layer_local, mesh=mesh,
                         in_specs=(row_spec, P('dp'), cache_spec, cache_spec, P(), col_spec, col_spec,
                                   col_spec, split_rows, P(), col_spec, col_spec, split_rows),
                         out_specs=(row_spec, cache_spec, cache_spec), check_vma=False)
```

```python
import functools
import math
import jax
import jax.numpy as jnp
import numpy as np
from jax import lax
from jax.experimental import pallas as pl
from jax.experimental.pallas import tpu as pltpu
from jax.sharding import PartitionSpec as P

EPS = 1e-5
ROPE_THETA = 500000.0
ROPE_FACTOR = 8.0
LOW_FACTOR = 1.0
HIGH_FACTOR = 4.0
ORIG_CTX = 8192.0

MESH = pl.DeviceIdType.MESH
BLK = 512
SLOTS = 11
SB = 8
UNROLL = 4
QCH = 5
LAG_D, LAG_1, LAG_2 = 2, 7, 17
GLAG_2, GLAG_3 = 3, 4
ZLAGS = (2, 6, 10, 14, 19, 21)


def rope_freqs(head_dim):
    exponents = np.arange(head_dim // 2) * (2.0 / head_dim)
    inv_freq = 1.0 / np.power(ROPE_THETA, exponents)
    wavelen = (2.0 * math.pi) / inv_freq
    smooth = (ORIG_CTX / wavelen - LOW_FACTOR) / (HIGH_FACTOR - LOW_FACTOR)
    blended = (1.0 - smooth) * inv_freq / ROPE_FACTOR + smooth * inv_freq
    inv_freq = np.where(wavelen < ORIG_CTX / HIGH_FACTOR, inv_freq,
                        np.where(wavelen > ORIG_CTX / LOW_FACTOR, inv_freq / ROPE_FACTOR, blended))
    return np.concatenate([inv_freq, inv_freq])[None].astype(np.float32)


def attn_kernel(pos_s, resid_hbm, gain_ref, pos_ref, freq_ref, wq_ref, wk_ref, wv_ref, kc_ref, vc_ref,
                out_ref, ko_ref, vo_ref, resid_ref, wqkv, kbuf, vbuf, normed, q_rot, k_rot, v_new, pos_b, o_buf,
                r_sem, q_sem, k_sem, v_sem, ko_sem, vo_sem):
    f32, bf16 = jnp.float32, jnp.bfloat16
    n_seqs, model = resid_ref.shape
    cache_len, dim = kbuf.shape[1], kbuf.shape[2]
    heads = wq_ref.shape[1] // dim
    width = heads * dim
    n_blk = n_seqs // SB
    kc = model // QCH

    def w_copies(i):
        sl = pl.ds(i * kc, kc)
        return [pltpu.make_async_copy(src.at[sl], wqkv.at[sl, pl.ds(at, size)], q_sem.at[i, j])
                for j, (src, at, size) in enumerate(((wq_ref, 0, width), (wk_ref, width, dim), (wv_ref, width + dim, dim)))]

    def seqs(i):
        return pl.ds(pl.multiple_of(i * SB, SB), SB)

    def k_in(i):
        return pltpu.make_async_copy(kc_ref.at[seqs(i)], kbuf.at[seqs(i)], k_sem.at[i])

    def v_in(i):
        return pltpu.make_async_copy(vc_ref.at[seqs(i)], vbuf.at[seqs(i)], v_sem.at[i])

    def k_out(i):
        return pltpu.make_async_copy(kbuf.at[seqs(i)], ko_ref.at[seqs(i)], ko_sem.at[i])

    def v_out(i):
        return pltpu.make_async_copy(vbuf.at[seqs(i)], vo_ref.at[seqs(i)], vo_sem.at[i])

    resid_copy = pltpu.make_async_copy(resid_hbm, resid_ref, r_sem)
    resid_copy.start()
    for c in w_copies(0) + w_copies(1):
        c.start()

    row_i = lax.broadcasted_iota(jnp.int32, (n_seqs, n_seqs), 0)
    col_i = lax.broadcasted_iota(jnp.int32, (n_seqs, n_seqs), 1)
    pos_f = pos_ref[...].astype(f32)
    pos_col = jnp.sum(jnp.where(row_i == col_i, pos_f, 0.0), axis=1, keepdims=True)
    pos_b[...] = jnp.broadcast_to(pos_col, pos_b.shape)
    angles = pos_b[...] * freq_ref[...]
    cos_t = jnp.cos(angles)
    lane = lax.broadcasted_iota(jnp.int32, angles.shape, 1)
    sin_t = jnp.sin(angles)
    sin_t = jnp.where(lane < dim // 2, -sin_t, sin_t)

    resid_copy.wait()
    for i in range(2, QCH):
        for c in w_copies(i):
            c.start()
    for i in range(n_blk):
        k_in(i).start()
        v_in(i).start()
    total = jnp.zeros((n_seqs, 1), f32)
    for i in range(QCH):
        x = resid_ref[:, i * kc:(i + 1) * kc].astype(f32)
        total += jnp.sum(x * x, axis=-1, keepdims=True)
    inv = lax.rsqrt(total * (1.0 / model) + EPS)
    for i in range(QCH):
        sl = slice(i * kc, (i + 1) * kc)
        normed[:, sl] = (resid_ref[:, sl].astype(f32) * inv * gain_ref[sl].astype(f32)[None]).astype(bf16)

    qkv = None
    for i in range(QCH):
        for c in w_copies(i):
            c.wait()
        sl = slice(i * kc, (i + 1) * kc)
        part = jnp.dot(normed[:, sl], wqkv[sl, :], preferred_element_type=f32)
        qkv = part if qkv is None else qkv + part

    def rope(x):
        x = x.astype(bf16).astype(f32)
        return (x * cos_t + pltpu.roll(x, dim // 2, 1) * sin_t).astype(bf16).astype(f32)

    for j in range(heads):
        q_rot[j] = rope(qkv[:, j * dim:(j + 1) * dim])
    k_rot[...] = rope(qkv[:, width:width + dim])
    v_new[...] = qkv[:, width + dim:].astype(bf16).astype(f32)

    pair = SB // 2
    rows, cols = heads * SB, pair * cache_len
    r_i = lax.rem(lax.broadcasted_iota(jnp.int32, (rows, cols), 0), SB)
    c_i = lax.broadcasted_iota(jnp.int32, (rows, cols), 1)
    slot_of = jnp.where(lax.rem(r_i, pair) == c_i // cache_len, lax.rem(c_i, cache_len), 2 * cache_len).astype(f32)
    early = lax.rem(lax.broadcasted_iota(jnp.int32, (rows, dim), 0), SB) < pair
    slot_row = lax.broadcasted_iota(jnp.int32, (cache_len, dim), 0).astype(f32).astype(bf16)
    scale = 1.0 / math.sqrt(dim)

    def both(buf, i):
        first = buf[pl.ds(pl.multiple_of(i * SB, pair), pair)].reshape(cols, dim)
        second = buf[pl.ds(pl.multiple_of(i * SB + pair, pair), pair)].reshape(cols, dim)
        return jnp.concatenate([first, second], axis=1)

    def block(i):
        k_in(i).wait()
        v_in(i).wait()
        for s in range(SB):
            n = i * SB + s
            hit = slot_row == jnp.full((cache_len, dim), pos_s[n].astype(f32)).astype(bf16)
            kbuf[n] = jnp.where(hit, jnp.broadcast_to(k_rot[pl.ds(n, 1), :], (cache_len, dim)).astype(bf16), kbuf[n])
            vbuf[n] = jnp.where(hit, jnp.broadcast_to(v_new[pl.ds(n, 1), :], (cache_len, dim)).astype(bf16), vbuf[n])
        k_out(i).start()
        v_out(i).start()
        q_b = jnp.concatenate([q_rot[j, seqs(i), :] for j in range(heads)], axis=0)
        q_b = jnp.concatenate([jnp.where(early, q_b, 0.0), jnp.where(early, 0.0, q_b)], axis=1).astype(bf16)
        sc = lax.dot_general(q_b, both(kbuf, i), (((1,), (1,)), ((), ())), preferred_element_type=f32) * scale
        p_b = jnp.concatenate([pos_b[seqs(i), :]] * heads, axis=0)
        p_b = jnp.concatenate([p_b] * pair, axis=1)
        sc = jnp.where(slot_of <= p_b, sc, -jnp.inf)
        ex = jnp.exp(sc - jnp.max(sc, axis=-1, keepdims=True))
        prob = (ex * (1.0 / jnp.sum(ex, axis=-1, keepdims=True))).astype(bf16)
        o = jnp.dot(prob, both(vbuf, i), preferred_element_type=f32)
        o = jnp.where(early, o[:, :dim], o[:, dim:])
        for j in range(heads):
            o_buf[seqs(i), j * dim:(j + 1) * dim] = o[j * SB:(j + 1) * SB]

    def step(g, c):
        for r in range(UNROLL):
            block(g * UNROLL + r)
        return c
    lax.fori_loop(0, n_blk // UNROLL, step, 0)
    out_ref[...] = o_buf[...].astype(bf16)

    def finish(i, c):
        k_out(i).wait()
        v_out(i).wait()
        return c
    lax.fori_loop(0, n_blk, finish, 0)


def attention_part(resid_in, positions, k_cache, v_cache, gain_attn, w_query, w_key, w_value):
    n_seqs, model = resid_in.shape
    cache_len, kv_heads, dim = k_cache.shape[1:]
    q_width = w_query.shape[1]
    f32, bf16 = jnp.float32, jnp.bfloat16
    cache_flat = (n_seqs, cache_len * kv_heads, dim)
    hbm = pl.BlockSpec(memory_space=pltpu.HBM)
    vmem = pl.BlockSpec(memory_space=pltpu.VMEM)
    smem = pl.BlockSpec(memory_space=pltpu.SMEM)
    n_blk = n_seqs // SB
    out, k_full, v_full = pl.pallas_call(
        attn_kernel,
        out_shape=(pltpu.VMEM((n_seqs, q_width), bf16), jax.ShapeDtypeStruct(cache_flat, bf16),
                   jax.ShapeDtypeStruct(cache_flat, bf16)),
        in_specs=[smem, hbm, vmem, vmem, vmem, hbm, hbm, hbm, hbm, hbm],
        out_specs=(vmem, hbm, hbm),
        scratch_shapes=[
            pltpu.VMEM((n_seqs, model), bf16), pltpu.VMEM((model, q_width + 2 * dim), bf16),
            pltpu.VMEM(cache_flat, bf16), pltpu.VMEM(cache_flat, bf16),
            pltpu.VMEM((n_seqs, model), bf16), pltpu.VMEM((q_width // dim, n_seqs, dim), f32),
            pltpu.VMEM((n_seqs, dim), f32), pltpu.VMEM((n_seqs, dim), f32), pltpu.VMEM((n_seqs, dim), f32),
            pltpu.VMEM((n_seqs, q_width), f32),
            pltpu.SemaphoreType.DMA, pltpu.SemaphoreType.DMA((QCH, 3)),
            pltpu.SemaphoreType.DMA((n_blk,)), pltpu.SemaphoreType.DMA((n_blk,)),
            pltpu.SemaphoreType.DMA((n_blk,)), pltpu.SemaphoreType.DMA((n_blk,)),
        ],
        compiler_params=pltpu.CompilerParams(vmem_limit_bytes=60_000_000),
        cost_estimate=pl.CostEstimate(flops=2 * n_seqs * model * q_width, bytes_accessed=30_000_000, transcendentals=0),
        name='attn',
    )(positions, resid_in, gain_attn, positions.reshape(1, n_seqs), rope_freqs(dim),
      w_query, w_key, w_value, k_cache.reshape(cache_flat), v_cache.reshape(cache_flat))
    return out, k_full.reshape(k_cache.shape), v_full.reshape(v_cache.shape)


def mlp_kernel(dims, o_ref, resid_ref, gain_ref, wo_ref, wg_ref, wu_ref, wd_ref, out_ref,
               ring, ybuf, r_d, r_1, r_2, hbuf, acc_g, acc_u, hidden, x_own, rows_own,
               w_sem, l_sem, snd, rcv):
    n_ch, n_fb, rows = dims
    me = lax.axis_index('tp')
    core = lax.rem(me, 2)
    chip = me // 2
    apair = chip // 2
    bpair = lax.rem((chip + 1) // 2, 2)
    chip_a = chip + 1 - 2 * lax.rem(chip, 2)
    chip_b = 3 - chip
    hi = bpair + core * (apair - bpair)
    lo = apair + core * (bpair - apair)
    first = 2 * (chip_a + core * (chip_b - chip_a)) + core
    second = 2 * (chip_b + core * (chip_a - chip_b)) + core
    mate = 2 * chip + 1 - core
    half = 4 * core
    own = half + 2 * hi + lo

    def remote(stage, u, src, dst, dev):
        return pltpu.make_async_remote_copy(src_ref=src, dst_ref=dst, send_sem=snd.at[stage, u], recv_sem=rcv.at[stage, u],
                                            device_id={'tp': dev}, device_id_type=MESH)

    def s_d(u):
        return remote(0, u, ybuf.at[u, pl.ds(4 - half, 4)], r_d.at[u], mate)

    def s_1(u):
        return remote(1, u, ybuf.at[u, pl.ds(half + 2 - 2 * hi, 2)], r_1.at[u], first)

    def s_2(u):
        return remote(2, u, ybuf.at[u, half + 2 * hi + 1 - lo], r_2.at[u], second)

    def g_1(u):
        return remote(3, u, hbuf.at[u, own], hbuf.at[u, own], second)

    def g_2(u):
        return remote(4, u, hbuf.at[u, pl.ds(half + 2 * hi, 2)], hbuf.at[u, pl.ds(half + 2 * hi, 2)], first)

    def g_3(u):
        return remote(5, u, hbuf.at[u, pl.ds(half, 4)], hbuf.at[u, pl.ds(half, 4)], mate)

    def load_out(b, slot, idx):
        return pltpu.make_async_copy(wo_ref.at[:, pl.ds(pl.multiple_of(b * BLK, BLK), BLK)], ring.at[slot, idx], w_sem.at[slot])

    def issue(load):
        slot = lax.rem(load, SLOTS)
        seq = load - 2

        def rows_of(w_ref, k):
            for b in range(n_fb):
                pltpu.make_async_copy(w_ref.at[pl.ds(pl.multiple_of(k * BLK, BLK), BLK), pl.ds(b * BLK, BLK)],
                                      ring.at[slot, b], w_sem.at[slot]).start()

        @pl.when((seq < 2 * n_ch) & (lax.rem(seq, 2) == 0))
        def _():
            rows_of(wg_ref, seq // 2)

        @pl.when((seq < 2 * n_ch) & (lax.rem(seq, 2) == 1))
        def _():
            rows_of(wu_ref, seq // 2)

        @pl.when((seq >= 2 * n_ch) & (seq < 3 * n_ch))
        def _():
            for b in range(n_fb):
                pltpu.make_async_copy(wd_ref.at[pl.ds(b * BLK, BLK), pl.ds(pl.multiple_of((seq - 2 * n_ch) * BLK, BLK), BLK)],
                                      ring.at[slot, b], w_sem.at[slot]).start()

    def wait_load(load):
        slot = lax.rem(load, SLOTS)
        pltpu.make_async_copy(ring.at[slot], ring.at[slot], w_sem.at[slot]).wait()
        return slot

    for b in range(n_fb):
        load_out(b, 0, b).start()
    for b in range(n_fb, n_ch):
        load_out(b, 1, b - n_fb).start()
    row_copy = pltpu.make_async_copy(resid_ref.at[pl.ds(pl.multiple_of(own * rows, rows), rows)], rows_own, l_sem)
    row_copy.start()

    def first_loads(i, c):
        issue(i)
        return c
    lax.fori_loop(2, SLOTS, first_loads, 0)

    barrier = pltpu.get_barrier_semaphore()
    for dev in (mate, first, second):
        pl.semaphore_signal(barrier, inc=1, device_id={'tp': dev}, device_id_type=MESH)
    pl.semaphore_wait(barrier, 3)

    def at(t, lag, fn):
        @pl.when((t >= lag) & (t < lag + n_ch))
        def _():
            fn(t - lag)

    def after_d(u):
        s_d(u).wait_recv()
        ybuf[u, pl.ds(half, 4)] += r_d[u]
        s_1(u).start()

    def after_1(u):
        s_1(u).wait_recv()
        ybuf[u, pl.ds(half + 2 * hi, 2)] += r_1[u]
        s_2(u).start()

    wait_load(0)
    pltpu.make_async_copy(ring.at[1, pl.ds(0, n_ch - n_fb)], ring.at[1, pl.ds(0, n_ch - n_fb)], w_sem.at[1]).wait()

    def step_y(t, c):
        def make(u):
            blk = ring[u // n_fb, lax.rem(u, n_fb)]
            y = jnp.dot(o_ref[...], blk, preferred_element_type=jnp.float32)
            ybuf[u] = y.reshape(8, rows, BLK)
            s_d(u).start()
        at(t, 0, make)

        @pl.when(t == n_ch)
        def _():
            issue(SLOTS)
            issue(SLOTS + 1)
        at(t, LAG_D, after_d)
        at(t, LAG_1, after_1)

        def done(u):
            s_2(u).wait_recv()
            x_own[u] = ybuf[u, own] + r_2[u]
        at(t, LAG_2, done)
        return c
    lax.fori_loop(0, n_ch + LAG_2, step_y, 0)

    def drain(u, c):
        s_d(u).wait_send()
        s_1(u).wait_send()
        s_2(u).wait_send()
        return c
    lax.fori_loop(0, n_ch, drain, 0)

    row_copy.wait()
    total = jnp.zeros((rows, 1), jnp.float32)
    for u in range(n_ch):
        x1 = (rows_own[:, u * BLK:(u + 1) * BLK].astype(jnp.float32) + x_own[u]).astype(jnp.bfloat16).astype(jnp.float32)
        x_own[u] = x1
        total += jnp.sum(x1 * x1, axis=-1, keepdims=True)
    inv = lax.rsqrt(total * (1.0 / (n_ch * BLK)) + EPS)
    for u in range(n_ch):
        gain = gain_ref[u * BLK:(u + 1) * BLK].astype(jnp.float32)[None]
        hbuf[u, own] = (x_own[u] * inv * gain).astype(jnp.bfloat16).astype(jnp.float32)
        g_1(u).start()

    acc_g[...] = jnp.zeros_like(acc_g)
    acc_u[...] = jnp.zeros_like(acc_u)

    def step_g(t, c):
        def fwd_1(u):
            g_1(u).wait_recv()
            g_2(u).start()
        at(t, 0, fwd_1)

        def fwd_2(u):
            g_2(u).wait_recv()
            g_3(u).start()
        at(t, GLAG_2, fwd_2)

        def compute(u):
            g_3(u).wait_recv()
            h_k = hbuf[u].reshape(8 * rows, BLK).astype(jnp.bfloat16)
            for which, acc in ((0, acc_g), (1, acc_u)):
                load = 2 + 2 * u + which
                slot = wait_load(load)
                for b in range(n_fb):
                    acc[b] += jnp.dot(h_k, ring[slot, b], preferred_element_type=jnp.float32)
                issue(load + SLOTS)
        at(t, GLAG_3, compute)
        return c
    lax.fori_loop(0, n_ch + GLAG_3, step_g, 0)

    def drain_g(u, c):
        g_1(u).wait_send()
        g_2(u).wait_send()
        g_3(u).wait_send()
        return c
    lax.fori_loop(0, n_ch, drain_g, 0)

    for b in range(n_fb):
        gate = acc_g[b].astype(jnp.bfloat16).astype(jnp.float32)
        up = acc_u[b].astype(jnp.bfloat16).astype(jnp.float32)
        hidden[:, b * BLK:(b + 1) * BLK] = (gate * jax.nn.sigmoid(gate) * up).astype(jnp.bfloat16)

    def step_z(t, c):
        def make(u):
            slot = wait_load(2 + 2 * n_ch + u)
            z = jnp.dot(hidden[...], ring[slot].reshape(n_fb * BLK, BLK), preferred_element_type=jnp.float32)
            ybuf[u] = z.reshape(8, rows, BLK)
            s_d(u).start()
        at(t, 0, make)
        at(t, ZLAGS[0], after_d)
        at(t, ZLAGS[1], after_1)

        def done(u):
            s_2(u).wait_recv()
            hbuf[u, own] = (x_own[u] + (ybuf[u, own] + r_2[u])).astype(jnp.bfloat16).astype(jnp.float32)
            g_1(u).start()
        at(t, ZLAGS[2], done)

        def fwd_1(u):
            g_1(u).wait_recv()
            g_2(u).start()
        at(t, ZLAGS[3], fwd_1)

        def fwd_2(u):
            g_2(u).wait_recv()
            g_3(u).start()
        at(t, ZLAGS[4], fwd_2)

        def write(u):
            g_3(u).wait_recv()
            out_ref[:, pl.ds(pl.multiple_of(u * BLK, BLK), BLK)] = hbuf[u].reshape(8 * rows, BLK).astype(jnp.bfloat16)
        at(t, ZLAGS[5], write)
        return c
    lax.fori_loop(0, n_ch + ZLAGS[5], step_z, 0)
    lax.fori_loop(0, n_ch, drain, 0)
    lax.fori_loop(0, n_ch, drain_g, 0)


def mlp_part(attn_out, resid_in, gain_mlp, w_out, w_gate, w_up, w_down):
    n_seqs, model = resid_in.shape
    ffn = w_gate.shape[1]
    n_ch, n_fb, rows = model // BLK, ffn // BLK, n_seqs // 8
    f32, bf16 = jnp.float32, jnp.bfloat16
    any_spec = pl.BlockSpec(memory_space=pltpu.HBM)
    vmem_spec = pl.BlockSpec(memory_space=pltpu.VMEM)
    return pl.pallas_call(
        functools.partial(mlp_kernel, (n_ch, n_fb, rows)),
        out_shape=pltpu.VMEM((n_seqs, model), bf16),
        in_specs=[vmem_spec, any_spec, vmem_spec, any_spec, any_spec, any_spec, any_spec],
        out_specs=vmem_spec,
        scratch_shapes=[
            pltpu.VMEM((SLOTS, n_fb, BLK, BLK), bf16),
            pltpu.VMEM((n_ch, 8, rows, BLK), f32),
            pltpu.VMEM((n_ch, 4, rows, BLK), f32),
            pltpu.VMEM((n_ch, 2, rows, BLK), f32),
            pltpu.VMEM((n_ch, rows, BLK), f32),
            pltpu.VMEM((n_ch, 8, rows, BLK), f32),
            pltpu.VMEM((n_fb, n_seqs, BLK), f32),
            pltpu.VMEM((n_fb, n_seqs, BLK), f32),
            pltpu.VMEM((n_seqs, ffn), bf16),
            pltpu.VMEM((n_ch, rows, BLK), f32),
            pltpu.VMEM((rows, model), bf16),
            pltpu.SemaphoreType.DMA((SLOTS,)),
            pltpu.SemaphoreType.DMA,
            pltpu.SemaphoreType.DMA((6, n_ch)),
            pltpu.SemaphoreType.DMA((6, n_ch)),
        ],
        compiler_params=pltpu.CompilerParams(collective_id=0, has_side_effects=True, vmem_limit_bytes=61_500_000),
        cost_estimate=pl.CostEstimate(flops=6 * n_seqs * model * ffn, bytes_accessed=6 * model * ffn, transcendentals=0),
        name='out_mlp',
    )(attn_out, resid_in, gain_mlp, w_out, w_gate, w_up, w_down)


def solution(mesh):
    def layer_local(resid_in, positions, k_cache, v_cache, gain_attn, w_query, w_key, w_value,
                    w_out, gain_mlp, w_gate, w_up, w_down):
        attn_out, k_full, v_full = attention_part(resid_in, positions, k_cache, v_cache,
                                                  gain_attn, w_query, w_key, w_value)
        resid_out = mlp_part(attn_out, resid_in, gain_mlp, w_out, w_gate, w_up, w_down)
        return resid_out, k_full, v_full

    row_spec = P('dp', None)
    cache_spec = P('dp', None, 'tp', None)
    col_spec = P(None, 'tp')
    split_rows = P('tp', None)
    return jax.shard_map(layer_local, mesh=mesh,
                         in_specs=(row_spec, P('dp'), cache_spec, cache_spec, P(), col_spec, col_spec,
                                   col_spec, split_rows, P(), col_spec, col_spec, split_rows),
                         out_specs=(row_spec, cache_spec, cache_spec), check_vma=False)
```

```python
import functools
import math
import jax
import jax.numpy as jnp
import numpy as np
from jax import lax
from jax.experimental import pallas as pl
from jax.experimental.pallas import tpu as pltpu
from jax.sharding import PartitionSpec as P

EPS = 1e-5
ROPE_THETA = 500000.0
ROPE_FACTOR = 8.0
LOW_FACTOR = 1.0
HIGH_FACTOR = 4.0
ORIG_CTX = 8192.0

MESH = pl.DeviceIdType.MESH
BLK = 512
SLOTS = 12
SB = 8
UNROLL = 4
QCH = 5
LAG_D, LAG_1, LAG_2 = 2, 7, 17
GLAG_2, GLAG_3 = 3, 4
ZLAGS = (2, 6, 10, 14, 19, 21)


def rope_freqs(head_dim):
    exponents = np.arange(head_dim // 2) * (2.0 / head_dim)
    inv_freq = 1.0 / np.power(ROPE_THETA, exponents)
    wavelen = (2.0 * math.pi) / inv_freq
    smooth = (ORIG_CTX / wavelen - LOW_FACTOR) / (HIGH_FACTOR - LOW_FACTOR)
    blended = (1.0 - smooth) * inv_freq / ROPE_FACTOR + smooth * inv_freq
    inv_freq = np.where(wavelen < ORIG_CTX / HIGH_FACTOR, inv_freq,
                        np.where(wavelen > ORIG_CTX / LOW_FACTOR, inv_freq / ROPE_FACTOR, blended))
    return np.concatenate([inv_freq, inv_freq])[None].astype(np.float32)


def attn_kernel(pos_s, resid_hbm, gain_ref, pos_ref, freq_ref, wq_ref, wk_ref, wv_ref, kc_ref, vc_ref,
                out_ref, ko_ref, vo_ref, resid_ref, wqkv, kbuf, vbuf, normed, q_rot, k_rot, v_new, pos_b, o_buf,
                r_sem, q_sem, k_sem, v_sem, ko_sem, vo_sem):
    f32, bf16 = jnp.float32, jnp.bfloat16
    n_seqs, model = resid_ref.shape
    cache_len, dim = kbuf.shape[1], kbuf.shape[2]
    heads = wq_ref.shape[1] // dim
    width = heads * dim
    n_blk = n_seqs // SB
    kc = model // QCH

    def w_copies(i):
        sl = pl.ds(i * kc, kc)
        return [pltpu.make_async_copy(src.at[sl], wqkv.at[sl, pl.ds(at, size)], q_sem.at[i, j])
                for j, (src, at, size) in enumerate(((wq_ref, 0, width), (wk_ref, width, dim), (wv_ref, width + dim, dim)))]

    def seqs(i):
        return pl.ds(pl.multiple_of(i * SB, SB), SB)

    def k_in(i):
        return pltpu.make_async_copy(kc_ref.at[seqs(i)], kbuf.at[seqs(i)], k_sem.at[i])

    def v_in(i):
        return pltpu.make_async_copy(vc_ref.at[seqs(i)], vbuf.at[seqs(i)], v_sem.at[i])

    def k_out(i):
        return pltpu.make_async_copy(kbuf.at[seqs(i)], ko_ref.at[seqs(i)], ko_sem.at[i])

    def v_out(i):
        return pltpu.make_async_copy(vbuf.at[seqs(i)], vo_ref.at[seqs(i)], vo_sem.at[i])

    resid_copy = pltpu.make_async_copy(resid_hbm, resid_ref, r_sem)
    resid_copy.start()
    for c in w_copies(0) + w_copies(1):
        c.start()

    row_i = lax.broadcasted_iota(jnp.int32, (n_seqs, n_seqs), 0)
    col_i = lax.broadcasted_iota(jnp.int32, (n_seqs, n_seqs), 1)
    pos_f = pos_ref[...].astype(f32)
    pos_col = jnp.sum(jnp.where(row_i == col_i, pos_f, 0.0), axis=1, keepdims=True)
    pos_b[...] = jnp.broadcast_to(pos_col, pos_b.shape)
    angles = pos_b[...] * freq_ref[...]
    cos_t = jnp.cos(angles)
    lane = lax.broadcasted_iota(jnp.int32, angles.shape, 1)
    sin_t = jnp.sin(angles)
    sin_t = jnp.where(lane < dim // 2, -sin_t, sin_t)

    resid_copy.wait()
    for i in range(2, QCH):
        for c in w_copies(i):
            c.start()
    for i in range(UNROLL):
        k_in(i).start()
        v_in(i).start()
    total = jnp.zeros((n_seqs, 1), f32)
    for i in range(QCH):
        x = resid_ref[:, i * kc:(i + 1) * kc].astype(f32)
        total += jnp.sum(x * x, axis=-1, keepdims=True)
    inv = lax.rsqrt(total * (1.0 / model) + EPS)
    for i in range(QCH):
        sl = slice(i * kc, (i + 1) * kc)
        normed[:, sl] = (resid_ref[:, sl].astype(f32) * inv * gain_ref[sl].astype(f32)[None]).astype(bf16)

    for i in range(UNROLL, n_blk):
        k_in(i).start()
        v_in(i).start()

    qkv = None
    for i in range(QCH):
        for c in w_copies(i):
            c.wait()
        sl = slice(i * kc, (i + 1) * kc)
        part = jnp.dot(normed[:, sl], wqkv[sl, :], preferred_element_type=f32)
        qkv = part if qkv is None else qkv + part

    def rope(x):
        x = x.astype(bf16).astype(f32)
        return (x * cos_t + pltpu.roll(x, dim // 2, 1) * sin_t).astype(bf16).astype(f32)

    for j in range(heads):
        q_rot[j] = rope(qkv[:, j * dim:(j + 1) * dim])
    k_rot[...] = rope(qkv[:, width:width + dim])
    v_new[...] = qkv[:, width + dim:].astype(bf16).astype(f32)

    pair = SB // 2
    rows, cols = heads * SB, pair * cache_len
    r_i = lax.rem(lax.broadcasted_iota(jnp.int32, (rows, cols), 0), SB)
    c_i = lax.broadcasted_iota(jnp.int32, (rows, cols), 1)
    slot_of = jnp.where(lax.rem(r_i, pair) == c_i // cache_len, lax.rem(c_i, cache_len), 2 * cache_len).astype(f32)
    early = lax.rem(lax.broadcasted_iota(jnp.int32, (rows, dim), 0), SB) < pair
    slot_row = lax.broadcasted_iota(jnp.int32, (cache_len, dim), 0).astype(f32).astype(bf16)
    scale = 1.0 / math.sqrt(dim)

    def both(buf, i):
        first = buf[pl.ds(pl.multiple_of(i * SB, pair), pair)].reshape(cols, dim)
        second = buf[pl.ds(pl.multiple_of(i * SB + pair, pair), pair)].reshape(cols, dim)
        return jnp.concatenate([first, second], axis=1)

    def update(i):
        for s in range(SB):
            n = i * SB + s
            hit = slot_row == jnp.full((cache_len, dim), pos_s[n].astype(f32)).astype(bf16)
            kbuf[n] = jnp.where(hit, jnp.broadcast_to(k_rot[pl.ds(n, 1), :], (cache_len, dim)).astype(bf16), kbuf[n])
            vbuf[n] = jnp.where(hit, jnp.broadcast_to(v_new[pl.ds(n, 1), :], (cache_len, dim)).astype(bf16), vbuf[n])

    def scores(i):
        q_b = jnp.concatenate([q_rot[j, seqs(i), :] for j in range(heads)], axis=0)
        q_b = jnp.concatenate([jnp.where(early, q_b, 0.0), jnp.where(early, 0.0, q_b)], axis=1).astype(bf16)
        return lax.dot_general(q_b, both(kbuf, i), (((1,), (1,)), ((), ())), preferred_element_type=f32) * scale

    def softmax(i, sc):
        p_b = jnp.concatenate([pos_b[seqs(i), :]] * heads, axis=0)
        p_b = jnp.concatenate([p_b] * pair, axis=1)
        sc = jnp.where(slot_of <= p_b, sc, -jnp.inf)
        ex = jnp.exp(sc - jnp.max(sc, axis=-1, keepdims=True))
        return (ex * (1.0 / jnp.sum(ex, axis=-1, keepdims=True))).astype(bf16)

    def step(g, c):
        blocks = [g * UNROLL + r for r in range(UNROLL)]
        for i in blocks:
            k_in(i).wait()
            v_in(i).wait()
        for i in blocks:
            update(i)
        for i in blocks:
            k_out(i).start()
            v_out(i).start()
        probs = [softmax(i, sc) for i, sc in [(i, scores(i)) for i in blocks]]
        outs = [jnp.dot(prob, both(vbuf, i), preferred_element_type=f32) for i, prob in zip(blocks, probs)]
        for i, o in zip(blocks, outs):
            o = jnp.where(early, o[:, :dim], o[:, dim:])
            for j in range(heads):
                o_buf[seqs(i), j * dim:(j + 1) * dim] = o[j * SB:(j + 1) * SB]
        return c
    lax.fori_loop(0, n_blk // UNROLL, step, 0)
    out_ref[...] = o_buf[...].astype(bf16)

    def finish(i, c):
        k_out(i).wait()
        v_out(i).wait()
        return c
    lax.fori_loop(0, n_blk, finish, 0)


def attention_part(resid_in, positions, k_cache, v_cache, gain_attn, w_query, w_key, w_value):
    n_seqs, model = resid_in.shape
    cache_len, kv_heads, dim = k_cache.shape[1:]
    q_width = w_query.shape[1]
    f32, bf16 = jnp.float32, jnp.bfloat16
    cache_flat = (n_seqs, cache_len * kv_heads, dim)
    hbm = pl.BlockSpec(memory_space=pltpu.HBM)
    vmem = pl.BlockSpec(memory_space=pltpu.VMEM)
    smem = pl.BlockSpec(memory_space=pltpu.SMEM)
    n_blk = n_seqs // SB
    out, k_full, v_full = pl.pallas_call(
        attn_kernel,
        out_shape=(pltpu.VMEM((n_seqs, q_width), bf16), jax.ShapeDtypeStruct(cache_flat, bf16),
                   jax.ShapeDtypeStruct(cache_flat, bf16)),
        in_specs=[smem, hbm, vmem, vmem, vmem, hbm, hbm, hbm, hbm, hbm],
        out_specs=(vmem, hbm, hbm),
        scratch_shapes=[
            pltpu.VMEM((n_seqs, model), bf16), pltpu.VMEM((model, q_width + 2 * dim), bf16),
            pltpu.VMEM(cache_flat, bf16), pltpu.VMEM(cache_flat, bf16),
            pltpu.VMEM((n_seqs, model), bf16), pltpu.VMEM((q_width // dim, n_seqs, dim), f32),
            pltpu.VMEM((n_seqs, dim), f32), pltpu.VMEM((n_seqs, dim), f32), pltpu.VMEM((n_seqs, dim), f32),
            pltpu.VMEM((n_seqs, q_width), f32),
            pltpu.SemaphoreType.DMA, pltpu.SemaphoreType.DMA((QCH, 3)),
            pltpu.SemaphoreType.DMA((n_blk,)), pltpu.SemaphoreType.DMA((n_blk,)),
            pltpu.SemaphoreType.DMA((n_blk,)), pltpu.SemaphoreType.DMA((n_blk,)),
        ],
        compiler_params=pltpu.CompilerParams(vmem_limit_bytes=60_000_000),
        cost_estimate=pl.CostEstimate(flops=2 * n_seqs * model * q_width, bytes_accessed=30_000_000, transcendentals=0),
        name='attn',
    )(positions, resid_in, gain_attn, positions.reshape(1, n_seqs), rope_freqs(dim),
      w_query, w_key, w_value, k_cache.reshape(cache_flat), v_cache.reshape(cache_flat))
    return out, k_full.reshape(k_cache.shape), v_full.reshape(v_cache.shape)


def mlp_kernel(dims, o_ref, resid_ref, gain_ref, wo_ref, wg_ref, wu_ref, wd_ref, out_ref,
               ring, ybuf, r_d, r_1, r_2, hbuf, acc_g, acc_u, hidden, x_own, rows_own,
               w_sem, l_sem, snd, rcv):
    n_ch, n_fb, rows = dims
    me = lax.axis_index('tp')
    core = lax.rem(me, 2)
    chip = me // 2
    apair = chip // 2
    bpair = lax.rem((chip + 1) // 2, 2)
    chip_a = chip + 1 - 2 * lax.rem(chip, 2)
    chip_b = 3 - chip
    hi = bpair + core * (apair - bpair)
    lo = apair + core * (bpair - apair)
    first = 2 * (chip_a + core * (chip_b - chip_a)) + core
    second = 2 * (chip_b + core * (chip_a - chip_b)) + core
    mate = 2 * chip + 1 - core
    half = 4 * core
    own = half + 2 * hi + lo

    def remote(stage, u, src, dst, dev):
        return pltpu.make_async_remote_copy(src_ref=src, dst_ref=dst, send_sem=snd.at[stage, u], recv_sem=rcv.at[stage, u],
                                            device_id={'tp': dev}, device_id_type=MESH)

    def s_d(u):
        return remote(0, u, ybuf.at[u, pl.ds(4 - half, 4)], r_d.at[u], mate)

    def s_1(u):
        return remote(1, u, ybuf.at[u, pl.ds(half + 2 - 2 * hi, 2)], r_1.at[u], first)

    def s_2(u):
        return remote(2, u, ybuf.at[u, half + 2 * hi + 1 - lo], r_2.at[u], second)

    def g_1(u):
        return remote(3, u, hbuf.at[u, own], hbuf.at[u, own], second)

    def g_2(u):
        return remote(4, u, hbuf.at[u, pl.ds(half + 2 * hi, 2)], hbuf.at[u, pl.ds(half + 2 * hi, 2)], first)

    def g_3(u):
        return remote(5, u, hbuf.at[u, pl.ds(half, 4)], hbuf.at[u, pl.ds(half, 4)], mate)

    def load_out(b, slot, idx):
        return pltpu.make_async_copy(wo_ref.at[:, pl.ds(pl.multiple_of(b * BLK, BLK), BLK)], ring.at[slot, idx], w_sem.at[slot])

    def issue(load):
        slot = lax.rem(load, SLOTS)
        seq = load - 2

        def rows_of(w_ref, k):
            for b in range(n_fb):
                pltpu.make_async_copy(w_ref.at[pl.ds(pl.multiple_of(k * BLK, BLK), BLK), pl.ds(b * BLK, BLK)],
                                      ring.at[slot, b], w_sem.at[slot]).start()

        @pl.when((seq < 2 * n_ch) & (lax.rem(seq, 2) == 0))
        def _():
            rows_of(wg_ref, seq // 2)

        @pl.when((seq < 2 * n_ch) & (lax.rem(seq, 2) == 1))
        def _():
            rows_of(wu_ref, seq // 2)

        @pl.when((seq >= 2 * n_ch) & (seq < 3 * n_ch))
        def _():
            for b in range(n_fb):
                pltpu.make_async_copy(wd_ref.at[pl.ds(b * BLK, BLK), pl.ds(pl.multiple_of((seq - 2 * n_ch) * BLK, BLK), BLK)],
                                      ring.at[slot, b], w_sem.at[slot]).start()

    def wait_load(load):
        slot = lax.rem(load, SLOTS)
        pltpu.make_async_copy(ring.at[slot], ring.at[slot], w_sem.at[slot]).wait()
        return slot

    for b in range(n_fb):
        load_out(b, 0, b).start()
    for b in range(n_fb, n_ch):
        load_out(b, 1, b - n_fb).start()
    row_copy = pltpu.make_async_copy(resid_ref.at[pl.ds(pl.multiple_of(own * rows, rows), rows)], rows_own, l_sem)
    row_copy.start()

    def first_loads(i, c):
        issue(i)
        return c
    lax.fori_loop(2, SLOTS, first_loads, 0)

    barrier = pltpu.get_barrier_semaphore()
    for dev in (mate, first, second):
        pl.semaphore_signal(barrier, inc=1, device_id={'tp': dev}, device_id_type=MESH)
    pl.semaphore_wait(barrier, 3)

    def at(t, lag, fn):
        @pl.when((t >= lag) & (t < lag + n_ch))
        def _():
            fn(t - lag)

    def after_d(u):
        s_d(u).wait_recv()
        ybuf[u, pl.ds(half, 4)] += r_d[u]
        s_1(u).start()

    def after_1(u):
        s_1(u).wait_recv()
        ybuf[u, pl.ds(half + 2 * hi, 2)] += r_1[u]
        s_2(u).start()

    wait_load(0)
    pltpu.make_async_copy(ring.at[1, pl.ds(0, n_ch - n_fb)], ring.at[1, pl.ds(0, n_ch - n_fb)], w_sem.at[1]).wait()

    def step_y(t, c):
        def make(u):
            blk = ring[u // n_fb, lax.rem(u, n_fb)]
            y = jnp.dot(o_ref[...], blk, preferred_element_type=jnp.float32)
            ybuf[u] = y.reshape(8, rows, BLK)
            s_d(u).start()
        at(t, 0, make)

        @pl.when(t == n_ch)
        def _():
            issue(SLOTS)
            issue(SLOTS + 1)
        at(t, LAG_D, after_d)
        at(t, LAG_1, after_1)

        def done(u):
            s_2(u).wait_recv()
            x_own[u] = ybuf[u, own] + r_2[u]
        at(t, LAG_2, done)
        return c
    lax.fori_loop(0, n_ch + LAG_2, step_y, 0)

    def drain(u, c):
        s_d(u).wait_send()
        s_1(u).wait_send()
        s_2(u).wait_send()
        return c
    lax.fori_loop(0, n_ch, drain, 0)

    row_copy.wait()
    total = jnp.zeros((rows, 1), jnp.float32)
    for u in range(n_ch):
        x1 = (rows_own[:, u * BLK:(u + 1) * BLK].astype(jnp.float32) + x_own[u]).astype(jnp.bfloat16).astype(jnp.float32)
        x_own[u] = x1
        total += jnp.sum(x1 * x1, axis=-1, keepdims=True)
    inv = lax.rsqrt(total * (1.0 / (n_ch * BLK)) + EPS)
    for u in range(n_ch):
        gain = gain_ref[u * BLK:(u + 1) * BLK].astype(jnp.float32)[None]
        hbuf[u, own] = (x_own[u] * inv * gain).astype(jnp.bfloat16).astype(jnp.float32)
        g_1(u).start()

    acc_g[...] = jnp.zeros_like(acc_g)
    acc_u[...] = jnp.zeros_like(acc_u)

    def step_g(t, c):
        def fwd_1(u):
            g_1(u).wait_recv()
            g_2(u).start()
        at(t, 0, fwd_1)

        def fwd_2(u):
            g_2(u).wait_recv()
            g_3(u).start()
        at(t, GLAG_2, fwd_2)

        def compute(u):
            g_3(u).wait_recv()
            h_k = hbuf[u].reshape(8 * rows, BLK).astype(jnp.bfloat16)
            for which, acc in ((0, acc_g), (1, acc_u)):
                slot = wait_load(2 + 2 * u + which)
                for b in range(n_fb):
                    acc[b] += jnp.dot(h_k, ring[slot, b], preferred_element_type=jnp.float32)
            issue(2 + 2 * u + SLOTS)
            issue(3 + 2 * u + SLOTS)
        at(t, GLAG_3, compute)
        return c
    lax.fori_loop(0, n_ch + GLAG_3, step_g, 0)

    def drain_g(u, c):
        g_1(u).wait_send()
        g_2(u).wait_send()
        g_3(u).wait_send()
        return c
    lax.fori_loop(0, n_ch, drain_g, 0)

    for b in range(n_fb):
        gate = acc_g[b].astype(jnp.bfloat16).astype(jnp.float32)
        up = acc_u[b].astype(jnp.bfloat16).astype(jnp.float32)
        hidden[:, b * BLK:(b + 1) * BLK] = (gate * jax.nn.sigmoid(gate) * up).astype(jnp.bfloat16)

    def step_z(t, c):
        def make(u):
            slot = wait_load(2 + 2 * n_ch + u)
            z = jnp.dot(hidden[...], ring[slot].reshape(n_fb * BLK, BLK), preferred_element_type=jnp.float32)
            ybuf[u] = z.reshape(8, rows, BLK)
            s_d(u).start()
        at(t, 0, make)
        at(t, ZLAGS[0], after_d)
        at(t, ZLAGS[1], after_1)

        def done(u):
            s_2(u).wait_recv()
            hbuf[u, own] = (x_own[u] + (ybuf[u, own] + r_2[u])).astype(jnp.bfloat16).astype(jnp.float32)
            g_1(u).start()
        at(t, ZLAGS[2], done)

        def fwd_1(u):
            g_1(u).wait_recv()
            g_2(u).start()
        at(t, ZLAGS[3], fwd_1)

        def fwd_2(u):
            g_2(u).wait_recv()
            g_3(u).start()
        at(t, ZLAGS[4], fwd_2)

        def write(u):
            g_3(u).wait_recv()
            out_ref[:, pl.ds(pl.multiple_of(u * BLK, BLK), BLK)] = hbuf[u].reshape(8 * rows, BLK).astype(jnp.bfloat16)
        at(t, ZLAGS[5], write)
        return c
    lax.fori_loop(0, n_ch + ZLAGS[5], step_z, 0)
    lax.fori_loop(0, n_ch, drain, 0)
    lax.fori_loop(0, n_ch, drain_g, 0)


def mlp_part(attn_out, resid_in, gain_mlp, w_out, w_gate, w_up, w_down):
    n_seqs, model = resid_in.shape
    ffn = w_gate.shape[1]
    n_ch, n_fb, rows = model // BLK, ffn // BLK, n_seqs // 8
    f32, bf16 = jnp.float32, jnp.bfloat16
    any_spec = pl.BlockSpec(memory_space=pltpu.HBM)
    vmem_spec = pl.BlockSpec(memory_space=pltpu.VMEM)
    return pl.pallas_call(
        functools.partial(mlp_kernel, (n_ch, n_fb, rows)),
        out_shape=pltpu.VMEM((n_seqs, model), bf16),
        in_specs=[vmem_spec, any_spec, vmem_spec, any_spec, any_spec, any_spec, any_spec],
        out_specs=vmem_spec,
        scratch_shapes=[
            pltpu.VMEM((SLOTS, n_fb, BLK, BLK), bf16),
            pltpu.VMEM((n_ch, 8, rows, BLK), f32),
            pltpu.VMEM((n_ch, 4, rows, BLK), f32),
            pltpu.VMEM((n_ch, 2, rows, BLK), f32),
            pltpu.VMEM((n_ch, rows, BLK), f32),
            pltpu.VMEM((n_ch, 8, rows, BLK), f32),
            pltpu.VMEM((n_fb, n_seqs, BLK), f32),
            pltpu.VMEM((n_fb, n_seqs, BLK), f32),
            pltpu.VMEM((n_seqs, ffn), bf16),
            pltpu.VMEM((n_ch, rows, BLK), f32),
            pltpu.VMEM((rows, model), bf16),
            pltpu.SemaphoreType.DMA((SLOTS,)),
            pltpu.SemaphoreType.DMA,
            pltpu.SemaphoreType.DMA((6, n_ch)),
            pltpu.SemaphoreType.DMA((6, n_ch)),
        ],
        compiler_params=pltpu.CompilerParams(collective_id=0, has_side_effects=True, vmem_limit_bytes=64_600_000),
        cost_estimate=pl.CostEstimate(flops=6 * n_seqs * model * ffn, bytes_accessed=6 * model * ffn, transcendentals=0),
        name='out_mlp',
    )(attn_out, resid_in, gain_mlp, w_out, w_gate, w_up, w_down)


def solution(mesh):
    def layer_local(resid_in, positions, k_cache, v_cache, gain_attn, w_query, w_key, w_value,
                    w_out, gain_mlp, w_gate, w_up, w_down):
        attn_out, k_full, v_full = attention_part(resid_in, positions, k_cache, v_cache,
                                                  gain_attn, w_query, w_key, w_value)
        attn_out = pltpu.with_memory_space_constraint(attn_out, pltpu.VMEM)
        resid_out = mlp_part(attn_out, resid_in, gain_mlp, w_out, w_gate, w_up, w_down)
        return resid_out, k_full, v_full

    row_spec = P('dp', None)
    cache_spec = P('dp', None, 'tp', None)
    col_spec = P(None, 'tp')
    split_rows = P('tp', None)
    return jax.shard_map(layer_local, mesh=mesh,
                         in_specs=(row_spec, P('dp'), cache_spec, cache_spec, P(), col_spec, col_spec,
                                   col_spec, split_rows, P(), col_spec, col_spec, split_rows),
                         out_specs=(row_spec, cache_spec, cache_spec), check_vma=False)
```

```python
import functools
import math
import jax
import jax.numpy as jnp
import numpy as np
from jax import lax
from jax.experimental import pallas as pl
from jax.experimental.pallas import tpu as pltpu
from jax.sharding import PartitionSpec as P

EPS = 1e-5
ROPE_THETA = 500000.0
ROPE_FACTOR = 8.0
LOW_FACTOR = 1.0
HIGH_FACTOR = 4.0
ORIG_CTX = 8192.0

MESH = pl.DeviceIdType.MESH
BLK = 512
SLOTS = 12
SB = 8
UNROLL = 8
QCH = 5
LAG_D, LAG_1, LAG_2 = 2, 7, 17
GLAG_2, GLAG_3 = 3, 4
ZLAGS = (2, 6, 10, 14, 19, 21)


def rope_freqs(head_dim):
    exponents = np.arange(head_dim // 2) * (2.0 / head_dim)
    inv_freq = 1.0 / np.power(ROPE_THETA, exponents)
    wavelen = (2.0 * math.pi) / inv_freq
    smooth = (ORIG_CTX / wavelen - LOW_FACTOR) / (HIGH_FACTOR - LOW_FACTOR)
    blended = (1.0 - smooth) * inv_freq / ROPE_FACTOR + smooth * inv_freq
    inv_freq = np.where(wavelen < ORIG_CTX / HIGH_FACTOR, inv_freq,
                        np.where(wavelen > ORIG_CTX / LOW_FACTOR, inv_freq / ROPE_FACTOR, blended))
    return np.concatenate([inv_freq, inv_freq])[None].astype(np.float32)


def attn_kernel(pos_s, resid_hbm, gain_ref, pos_ref, freq_ref, wq_ref, wk_ref, wv_ref, kc_ref, vc_ref,
                out_ref, ko_ref, vo_ref, resid_ref, wqkv, kbuf, vbuf, normed, q_rot, k_rot, v_new, pos_b, o_buf,
                r_sem, q_sem, k_sem, v_sem, ko_sem, vo_sem):
    f32, bf16 = jnp.float32, jnp.bfloat16
    n_seqs, model = resid_ref.shape
    cache_len, dim = kbuf.shape[1], kbuf.shape[2]
    heads = wq_ref.shape[1] // dim
    width = heads * dim
    n_blk = n_seqs // SB
    kc = model // QCH

    def w_copies(i):
        sl = pl.ds(i * kc, kc)
        return [pltpu.make_async_copy(src.at[sl], wqkv.at[sl, pl.ds(at, size)], q_sem.at[i, j])
                for j, (src, at, size) in enumerate(((wq_ref, 0, width), (wk_ref, width, dim), (wv_ref, width + dim, dim)))]

    def seqs(i):
        return pl.ds(pl.multiple_of(i * SB, SB), SB)

    def k_in(i):
        return pltpu.make_async_copy(kc_ref.at[seqs(i)], kbuf.at[seqs(i)], k_sem.at[i])

    def v_in(i):
        return pltpu.make_async_copy(vc_ref.at[seqs(i)], vbuf.at[seqs(i)], v_sem.at[i])

    def k_out(i):
        return pltpu.make_async_copy(kbuf.at[seqs(i)], ko_ref.at[seqs(i)], ko_sem.at[i])

    def v_out(i):
        return pltpu.make_async_copy(vbuf.at[seqs(i)], vo_ref.at[seqs(i)], vo_sem.at[i])

    resid_copy = pltpu.make_async_copy(resid_hbm, resid_ref, r_sem)
    resid_copy.start()
    for c in w_copies(0) + w_copies(1):
        c.start()

    row_i = lax.broadcasted_iota(jnp.int32, (n_seqs, n_seqs), 0)
    col_i = lax.broadcasted_iota(jnp.int32, (n_seqs, n_seqs), 1)
    pos_f = pos_ref[...].astype(f32)
    pos_col = jnp.sum(jnp.where(row_i == col_i, pos_f, 0.0), axis=1, keepdims=True)
    pos_b[...] = jnp.broadcast_to(pos_col, pos_b.shape)
    angles = pos_b[...] * freq_ref[...]
    cos_t = jnp.cos(angles)
    lane = lax.broadcasted_iota(jnp.int32, angles.shape, 1)
    sin_t = jnp.sin(angles)
    sin_t = jnp.where(lane < dim // 2, -sin_t, sin_t)

    resid_copy.wait()
    for i in range(2, QCH):
        for c in w_copies(i):
            c.start()
    total = jnp.zeros((n_seqs, 1), f32)
    for i in range(QCH):
        x = resid_ref[:, i * kc:(i + 1) * kc].astype(f32)
        total += jnp.sum(x * x, axis=-1, keepdims=True)
    inv = lax.rsqrt(total * (1.0 / model) + EPS)
    for i in range(QCH):
        sl = slice(i * kc, (i + 1) * kc)
        normed[:, sl] = (resid_ref[:, sl].astype(f32) * inv * gain_ref[sl].astype(f32)[None]).astype(bf16)

    for i in range(n_blk):
        k_in(i).start()
        v_in(i).start()

    qkv = None
    for i in range(QCH):
        for c in w_copies(i):
            c.wait()
        sl = slice(i * kc, (i + 1) * kc)
        part = jnp.dot(normed[:, sl], wqkv[sl, :], preferred_element_type=f32)
        qkv = part if qkv is None else qkv + part

    def rope(x):
        x = x.astype(bf16).astype(f32)
        return (x * cos_t + pltpu.roll(x, dim // 2, 1) * sin_t).astype(bf16).astype(f32)

    for j in range(heads):
        q_rot[j] = rope(qkv[:, j * dim:(j + 1) * dim])
    k_rot[...] = rope(qkv[:, width:width + dim])
    v_new[...] = qkv[:, width + dim:].astype(bf16).astype(f32)

    pair = SB // 2
    rows, cols = heads * SB, pair * cache_len
    r_i = lax.rem(lax.broadcasted_iota(jnp.int32, (rows, cols), 0), SB)
    c_i = lax.broadcasted_iota(jnp.int32, (rows, cols), 1)
    slot_of = jnp.where(lax.rem(r_i, pair) == c_i // cache_len, lax.rem(c_i, cache_len), 2 * cache_len).astype(f32)
    early = lax.rem(lax.broadcasted_iota(jnp.int32, (rows, dim), 0), SB) < pair
    slot_row = lax.broadcasted_iota(jnp.int32, (cache_len, dim), 0).astype(f32).astype(bf16)
    scale = 1.0 / math.sqrt(dim)

    def both(buf, i):
        first = buf[pl.ds(pl.multiple_of(i * SB, pair), pair)].reshape(cols, dim)
        second = buf[pl.ds(pl.multiple_of(i * SB + pair, pair), pair)].reshape(cols, dim)
        return jnp.concatenate([first, second], axis=1)

    def update(i):
        for s in range(SB):
            n = i * SB + s
            hit = slot_row == jnp.full((cache_len, dim), pos_s[n].astype(f32)).astype(bf16)
            kbuf[n] = jnp.where(hit, jnp.broadcast_to(k_rot[pl.ds(n, 1), :], (cache_len, dim)).astype(bf16), kbuf[n])
            vbuf[n] = jnp.where(hit, jnp.broadcast_to(v_new[pl.ds(n, 1), :], (cache_len, dim)).astype(bf16), vbuf[n])

    def scores(i):
        q_b = jnp.concatenate([q_rot[j, seqs(i), :] for j in range(heads)], axis=0)
        q_b = jnp.concatenate([jnp.where(early, q_b, 0.0), jnp.where(early, 0.0, q_b)], axis=1).astype(bf16)
        return lax.dot_general(q_b, both(kbuf, i), (((1,), (1,)), ((), ())), preferred_element_type=f32) * scale

    def softmax(i, sc):
        p_b = jnp.concatenate([pos_b[seqs(i), :]] * heads, axis=0)
        p_b = jnp.concatenate([p_b] * pair, axis=1)
        sc = jnp.where(slot_of <= p_b, sc, -jnp.inf)
        ex = jnp.exp(sc - jnp.max(sc, axis=-1, keepdims=True))
        return (ex * (1.0 / jnp.sum(ex, axis=-1, keepdims=True))).astype(bf16)

    def step(g, c):
        blocks = [g * UNROLL + r for r in range(UNROLL)]
        for i in blocks:
            k_in(i).wait()
            v_in(i).wait()
        for i in blocks:
            update(i)
        for i in blocks:
            k_out(i).start()
            v_out(i).start()
        probs = [softmax(i, sc) for i, sc in [(i, scores(i)) for i in blocks]]
        outs = [jnp.dot(prob, both(vbuf, i), preferred_element_type=f32) for i, prob in zip(blocks, probs)]
        for i, o in zip(blocks, outs):
            o = jnp.where(early, o[:, :dim], o[:, dim:])
            for j in range(heads):
                o_buf[seqs(i), j * dim:(j + 1) * dim] = o[j * SB:(j + 1) * SB]
        return c
    lax.fori_loop(0, n_blk // UNROLL, step, 0)
    out_ref[...] = o_buf[...].astype(bf16)

    def finish(i, c):
        k_out(i).wait()
        v_out(i).wait()
        return c
    lax.fori_loop(0, n_blk, finish, 0)


def attention_part(resid_in, positions, k_cache, v_cache, gain_attn, w_query, w_key, w_value):
    n_seqs, model = resid_in.shape
    cache_len, kv_heads, dim = k_cache.shape[1:]
    q_width = w_query.shape[1]
    f32, bf16 = jnp.float32, jnp.bfloat16
    cache_flat = (n_seqs, cache_len * kv_heads, dim)
    hbm = pl.BlockSpec(memory_space=pltpu.HBM)
    vmem = pl.BlockSpec(memory_space=pltpu.VMEM)
    smem = pl.BlockSpec(memory_space=pltpu.SMEM)
    n_blk = n_seqs // SB
    out, k_full, v_full = pl.pallas_call(
        attn_kernel,
        out_shape=(pltpu.VMEM((n_seqs, q_width), bf16), jax.ShapeDtypeStruct(cache_flat, bf16),
                   jax.ShapeDtypeStruct(cache_flat, bf16)),
        in_specs=[smem, hbm, vmem, vmem, vmem, hbm, hbm, hbm, hbm, hbm],
        out_specs=(vmem, hbm, hbm),
        scratch_shapes=[
            pltpu.VMEM((n_seqs, model), bf16), pltpu.VMEM((model, q_width + 2 * dim), bf16),
            pltpu.VMEM(cache_flat, bf16), pltpu.VMEM(cache_flat, bf16),
            pltpu.VMEM((n_seqs, model), bf16), pltpu.VMEM((q_width // dim, n_seqs, dim), f32),
            pltpu.VMEM((n_seqs, dim), f32), pltpu.VMEM((n_seqs, dim), f32), pltpu.VMEM((n_seqs, dim), f32),
            pltpu.VMEM((n_seqs, q_width), f32),
            pltpu.SemaphoreType.DMA, pltpu.SemaphoreType.DMA((QCH, 3)),
            pltpu.SemaphoreType.DMA((n_blk,)), pltpu.SemaphoreType.DMA((n_blk,)),
            pltpu.SemaphoreType.DMA((n_blk,)), pltpu.SemaphoreType.DMA((n_blk,)),
        ],
        compiler_params=pltpu.CompilerParams(vmem_limit_bytes=60_000_000),
        cost_estimate=pl.CostEstimate(flops=2 * n_seqs * model * q_width, bytes_accessed=30_000_000, transcendentals=0),
        name='attn',
    )(positions, resid_in, gain_attn, positions.reshape(1, n_seqs), rope_freqs(dim),
      w_query, w_key, w_value, k_cache.reshape(cache_flat), v_cache.reshape(cache_flat))
    return out, k_full.reshape(k_cache.shape), v_full.reshape(v_cache.shape)


def mlp_kernel(dims, o_ref, resid_ref, gain_ref, wo_ref, wg_ref, wu_ref, wd_ref, out_ref,
               ring, ybuf, r_d, r_1, r_2, hbuf, acc_g, acc_u, hidden, x_own, rows_own,
               w_sem, l_sem, snd, rcv):
    n_ch, n_fb, rows = dims
    me = lax.axis_index('tp')
    core = lax.rem(me, 2)
    chip = me // 2
    apair = chip // 2
    bpair = lax.rem((chip + 1) // 2, 2)
    chip_a = chip + 1 - 2 * lax.rem(chip, 2)
    chip_b = 3 - chip
    hi = bpair + core * (apair - bpair)
    lo = apair + core * (bpair - apair)
    first = 2 * (chip_a + core * (chip_b - chip_a)) + core
    second = 2 * (chip_b + core * (chip_a - chip_b)) + core
    mate = 2 * chip + 1 - core
    half = 4 * core
    own = half + 2 * hi + lo

    def remote(stage, u, src, dst, dev):
        return pltpu.make_async_remote_copy(src_ref=src, dst_ref=dst, send_sem=snd.at[stage, u], recv_sem=rcv.at[stage, u],
                                            device_id={'tp': dev}, device_id_type=MESH)

    def s_d(u):
        return remote(0, u, ybuf.at[u, pl.ds(4 - half, 4)], r_d.at[u], mate)

    def s_1(u):
        return remote(1, u, ybuf.at[u, pl.ds(half + 2 - 2 * hi, 2)], r_1.at[u], first)

    def s_2(u):
        return remote(2, u, ybuf.at[u, half + 2 * hi + 1 - lo], r_2.at[u], second)

    def g_1(u):
        return remote(3, u, hbuf.at[u, own], hbuf.at[u, own], second)

    def g_2(u):
        return remote(4, u, hbuf.at[u, pl.ds(half + 2 * hi, 2)], hbuf.at[u, pl.ds(half + 2 * hi, 2)], first)

    def g_3(u):
        return remote(5, u, hbuf.at[u, pl.ds(half, 4)], hbuf.at[u, pl.ds(half, 4)], mate)

    def load_out(b, slot, idx):
        return pltpu.make_async_copy(wo_ref.at[:, pl.ds(pl.multiple_of(b * BLK, BLK), BLK)], ring.at[slot, idx], w_sem.at[slot])

    def issue(load):
        slot = lax.rem(load, SLOTS)
        seq = load - 2

        def rows_of(w_ref, k):
            for b in range(n_fb):
                pltpu.make_async_copy(w_ref.at[pl.ds(pl.multiple_of(k * BLK, BLK), BLK), pl.ds(b * BLK, BLK)],
                                      ring.at[slot, b], w_sem.at[slot]).start()

        @pl.when((seq < 2 * n_ch) & (lax.rem(seq, 2) == 0))
        def _():
            rows_of(wg_ref, seq // 2)

        @pl.when((seq < 2 * n_ch) & (lax.rem(seq, 2) == 1))
        def _():
            rows_of(wu_ref, seq // 2)

        @pl.when((seq >= 2 * n_ch) & (seq < 3 * n_ch))
        def _():
            for b in range(n_fb):
                pltpu.make_async_copy(wd_ref.at[pl.ds(b * BLK, BLK), pl.ds(pl.multiple_of((seq - 2 * n_ch) * BLK, BLK), BLK)],
                                      ring.at[slot, b], w_sem.at[slot]).start()

    def wait_load(load):
        slot = lax.rem(load, SLOTS)
        pltpu.make_async_copy(ring.at[slot], ring.at[slot], w_sem.at[slot]).wait()
        return slot

    barrier = pltpu.get_barrier_semaphore()
    for dev in (mate, first, second):
        pl.semaphore_signal(barrier, inc=1, device_id={'tp': dev}, device_id_type=MESH)

    for b in range(n_fb):
        load_out(b, 0, b).start()
    for b in range(n_fb, n_ch):
        load_out(b, 1, b - n_fb).start()
    row_copy = pltpu.make_async_copy(resid_ref.at[pl.ds(pl.multiple_of(own * rows, rows), rows)], rows_own, l_sem)
    row_copy.start()

    def first_loads(i, c):
        issue(i)
        return c
    lax.fori_loop(2, SLOTS, first_loads, 0)

    pl.semaphore_wait(barrier, 3)

    def at(t, lag, fn):
        @pl.when((t >= lag) & (t < lag + n_ch))
        def _():
            fn(t - lag)

    def after_d(u):
        s_d(u).wait_recv()
        ybuf[u, pl.ds(half, 4)] += r_d[u]
        s_1(u).start()

    def after_1(u):
        s_1(u).wait_recv()
        ybuf[u, pl.ds(half + 2 * hi, 2)] += r_1[u]
        s_2(u).start()

    wait_load(0)
    pltpu.make_async_copy(ring.at[1, pl.ds(0, n_ch - n_fb)], ring.at[1, pl.ds(0, n_ch - n_fb)], w_sem.at[1]).wait()

    def step_y(t, c):
        def make(u):
            blk = ring[u // n_fb, lax.rem(u, n_fb)]
            y = jnp.dot(o_ref[...], blk, preferred_element_type=jnp.float32)
            ybuf[u] = y.reshape(8, rows, BLK)
            s_d(u).start()
        at(t, 0, make)

        @pl.when(t == n_ch)
        def _():
            issue(SLOTS)
            issue(SLOTS + 1)
        at(t, LAG_D, after_d)
        at(t, LAG_1, after_1)

        def done(u):
            s_2(u).wait_recv()
            x_own[u] = ybuf[u, own] + r_2[u]
        at(t, LAG_2, done)
        return c
    lax.fori_loop(0, n_ch + LAG_2, step_y, 0)

    def drain(u, c):
        s_d(u).wait_send()
        s_1(u).wait_send()
        s_2(u).wait_send()
        return c
    lax.fori_loop(0, n_ch, drain, 0)

    row_copy.wait()
    total = jnp.zeros((rows, 1), jnp.float32)
    for u in range(n_ch):
        x1 = (rows_own[:, u * BLK:(u + 1) * BLK].astype(jnp.float32) + x_own[u]).astype(jnp.bfloat16).astype(jnp.float32)
        x_own[u] = x1
        total += jnp.sum(x1 * x1, axis=-1, keepdims=True)
    inv = lax.rsqrt(total * (1.0 / (n_ch * BLK)) + EPS)
    for u in range(n_ch):
        gain = gain_ref[u * BLK:(u + 1) * BLK].astype(jnp.float32)[None]
        hbuf[u, own] = (x_own[u] * inv * gain).astype(jnp.bfloat16).astype(jnp.float32)
        g_1(u).start()

    acc_g[...] = jnp.zeros_like(acc_g)
    acc_u[...] = jnp.zeros_like(acc_u)

    def step_g(t, c):
        def fwd_1(u):
            g_1(u).wait_recv()
            g_2(u).start()
        at(t, 0, fwd_1)

        def fwd_2(u):
            g_2(u).wait_recv()
            g_3(u).start()
        at(t, GLAG_2, fwd_2)

        def compute(u):
            g_3(u).wait_recv()
            h_k = hbuf[u].reshape(8 * rows, BLK).astype(jnp.bfloat16)
            for which, acc in ((0, acc_g), (1, acc_u)):
                slot = wait_load(2 + 2 * u + which)
                for b in range(n_fb):
                    acc[b] += jnp.dot(h_k, ring[slot, b], preferred_element_type=jnp.float32)
            issue(2 + 2 * u + SLOTS)
            issue(3 + 2 * u + SLOTS)
        at(t, GLAG_3, compute)
        return c
    lax.fori_loop(0, n_ch + GLAG_3, step_g, 0)

    def drain_g(u, c):
        g_1(u).wait_send()
        g_2(u).wait_send()
        g_3(u).wait_send()
        return c
    lax.fori_loop(0, n_ch, drain_g, 0)

    for b in range(n_fb):
        gate = acc_g[b].astype(jnp.bfloat16).astype(jnp.float32)
        up = acc_u[b].astype(jnp.bfloat16).astype(jnp.float32)
        hidden[:, b * BLK:(b + 1) * BLK] = (gate * jax.nn.sigmoid(gate) * up).astype(jnp.bfloat16)

    def step_z(t, c):
        def make(u):
            slot = wait_load(2 + 2 * n_ch + u)
            z = jnp.dot(hidden[...], ring[slot].reshape(n_fb * BLK, BLK), preferred_element_type=jnp.float32)
            ybuf[u] = z.reshape(8, rows, BLK)
            s_d(u).start()
        at(t, 0, make)
        at(t, ZLAGS[0], after_d)
        at(t, ZLAGS[1], after_1)

        def done(u):
            s_2(u).wait_recv()
            hbuf[u, own] = (x_own[u] + (ybuf[u, own] + r_2[u])).astype(jnp.bfloat16).astype(jnp.float32)
            g_1(u).start()
        at(t, ZLAGS[2], done)

        def fwd_1(u):
            g_1(u).wait_recv()
            g_2(u).start()
        at(t, ZLAGS[3], fwd_1)

        def fwd_2(u):
            g_2(u).wait_recv()
            g_3(u).start()
        at(t, ZLAGS[4], fwd_2)

        def write(u):
            g_3(u).wait_recv()
            out_ref[:, pl.ds(pl.multiple_of(u * BLK, BLK), BLK)] = hbuf[u].reshape(8 * rows, BLK).astype(jnp.bfloat16)
        at(t, ZLAGS[5], write)
        return c
    lax.fori_loop(0, n_ch + ZLAGS[5], step_z, 0)
    lax.fori_loop(0, n_ch, drain, 0)
    lax.fori_loop(0, n_ch, drain_g, 0)


def mlp_part(attn_out, resid_in, gain_mlp, w_out, w_gate, w_up, w_down):
    n_seqs, model = resid_in.shape
    ffn = w_gate.shape[1]
    n_ch, n_fb, rows = model // BLK, ffn // BLK, n_seqs // 8
    f32, bf16 = jnp.float32, jnp.bfloat16
    any_spec = pl.BlockSpec(memory_space=pltpu.HBM)
    vmem_spec = pl.BlockSpec(memory_space=pltpu.VMEM)
    return pl.pallas_call(
        functools.partial(mlp_kernel, (n_ch, n_fb, rows)),
        out_shape=pltpu.VMEM((n_seqs, model), bf16),
        in_specs=[vmem_spec, any_spec, vmem_spec, any_spec, any_spec, any_spec, any_spec],
        out_specs=vmem_spec,
        scratch_shapes=[
            pltpu.VMEM((SLOTS, n_fb, BLK, BLK), bf16),
            pltpu.VMEM((n_ch, 8, rows, BLK), f32),
            pltpu.VMEM((n_ch, 4, rows, BLK), f32),
            pltpu.VMEM((n_ch, 2, rows, BLK), f32),
            pltpu.VMEM((n_ch, rows, BLK), f32),
            pltpu.VMEM((n_ch, 8, rows, BLK), f32),
            pltpu.VMEM((n_fb, n_seqs, BLK), f32),
            pltpu.VMEM((n_fb, n_seqs, BLK), f32),
            pltpu.VMEM((n_seqs, ffn), bf16),
            pltpu.VMEM((n_ch, rows, BLK), f32),
            pltpu.VMEM((rows, model), bf16),
            pltpu.SemaphoreType.DMA((SLOTS,)),
            pltpu.SemaphoreType.DMA,
            pltpu.SemaphoreType.DMA((6, n_ch)),
            pltpu.SemaphoreType.DMA((6, n_ch)),
        ],
        compiler_params=pltpu.CompilerParams(collective_id=0, has_side_effects=True, vmem_limit_bytes=64_600_000),
        cost_estimate=pl.CostEstimate(flops=6 * n_seqs * model * ffn, bytes_accessed=6 * model * ffn, transcendentals=0),
        name='out_mlp',
    )(attn_out, resid_in, gain_mlp, w_out, w_gate, w_up, w_down)


def solution(mesh):
    def layer_local(resid_in, positions, k_cache, v_cache, gain_attn, w_query, w_key, w_value,
                    w_out, gain_mlp, w_gate, w_up, w_down):
        attn_out, k_full, v_full = attention_part(resid_in, positions, k_cache, v_cache,
                                                  gain_attn, w_query, w_key, w_value)
        attn_out = pltpu.with_memory_space_constraint(attn_out, pltpu.VMEM)
        resid_out = mlp_part(attn_out, resid_in, gain_mlp, w_out, w_gate, w_up, w_down)
        return resid_out, k_full, v_full

    row_spec = P('dp', None)
    cache_spec = P('dp', None, 'tp', None)
    col_spec = P(None, 'tp')
    split_rows = P('tp', None)
    return jax.shard_map(layer_local, mesh=mesh,
                         in_specs=(row_spec, P('dp'), cache_spec, cache_spec, P(), col_spec, col_spec,
                                   col_spec, split_rows, P(), col_spec, col_spec, split_rows),
                         out_specs=(row_spec, cache_spec, cache_spec), check_vma=False)
```
